512 devices in a mesh: orb: 4 (over x), gx: 8 (over y), gyz: 16 (over z, core).
Axes of the slice: x: 4, y: 8, z: 8, core: 2. Of those that a mesh axis runs over, the one named last changes fastest.
Arguments:
- orbitals: float32 [2, 12, 128, 128, 128], P(None, 'orb', 'gx', 'gyz'), parts along dimension 1, may hold values from -12 to 12
- potential: float32 [128, 128, 128], P('gx', 'gyz'), may hold values from -8 to 60
Outputs:
- evolved: float32 [2, 12, 128, 128, 128], P(None, 'orb', 'gx', 'gyz'), parts along dimension 1
- residual: float32 [2, 12, 128, 128, 128], P(None, 'orb', 'gx', 'gyz'), parts along dimension 1
The draws below stay inside these ranges and needn't reach their ends.
There are 4 independent parts, one for each index of `orb`. The reference program is written for one: setup_inputs(seed, part) draws one part's arguments, and reference() takes and returns one part's arrays. A program takes and returns all parts, laid end to end along the dimension named above; an argument that names none is the same for every part. Nothing has to cross between parts.
All inputs are finite; a program needn't handle non-finite values.
Results may differ from the reference program's by a relative error of at most 0.0003.
Values sent between devices are 32-bit elements; how exact they have to be, the bound alone decides.
A program may use at most 64 MiB of HBM per device.

```python
import jax
import jax.numpy as jnp

ORB = 3
NZ = 128
ITERS = 4
NX = 128
NY = 128


def draw_orbitals(key, part):
    shape = (2, ORB, NX, NY, NZ)
    ramp = 1.0 + 2.0 * jnp.arange(NX, dtype=jnp.float32) / (NX - 1)
    envelope = ramp[None, None, :, None, None]
    values = jax.random.normal(jax.random.fold_in(key, 13), shape, jnp.float32)
    return jnp.clip(values, -4.0, 4.0) * envelope


def draw_potential(key, part):
    rough = jax.random.uniform(jax.random.fold_in(key, 21), (NX, NY, NZ), jnp.float32, -8.0, 8.0)
    ramp = 40.0 * jnp.arange(NX, dtype=jnp.float32)[:, None, None] / (NX - 1)
    return rough + ramp


def setup_inputs(seed: int = 0, part: int = 0) -> dict:
    splits = jax.random.split(jax.random.key(seed), 3)
    own_keys = jax.random.split(jax.random.fold_in(splits[2], part), 3)
    return {
        "orbitals": draw_orbitals(jax.random.fold_in(jax.random.fold_in(splits[2], part), 71), part),
        "potential": draw_potential(jax.random.fold_in(splits[2], 71), part),
    }


SPACING = 0.25
HALF_STEP = 0.05
COEFF_NEAR = 4.0 / 3.0
COEFF_FAR = -1.0 / 12.0
COEFF_SELF = -2.5


def laplace_apply(padded, potential):
    extent = (padded.shape[2] - 4, padded.shape[3] - 4, padded.shape[4] - 4)

    def window(shift_x, shift_y, shift_z):
        return padded[:, :, 2 + shift_x:2 + shift_x + extent[0], 2 + shift_y:2 + shift_y + extent[1], 2 + shift_z:2 + shift_z + extent[2]]

    center = window(0, 0, 0)
    summed = (3.0 * COEFF_SELF) * center
    for offset, weight in ((1, COEFF_NEAR), (2, COEFF_FAR)):
        summed = summed + weight * (window(offset, 0, 0) + window(-offset, 0, 0) + window(0, offset, 0) + window(0, -offset, 0) + window(0, 0, offset) + window(0, 0, -offset))
    return (-0.5 / SPACING ** 2) * summed + potential * center


def hamiltonian(vector, potential):
    padded = jnp.pad(vector, ((0, 0), (0, 0), (2, 2), (2, 2), (2, 2)))
    return laplace_apply(padded, potential)


def system(vector, applied):
    return jnp.stack([vector[0] - HALF_STEP * applied[1], vector[1] + HALF_STEP * applied[0]])


def precondition(vector, potential):
    diagonal = HALF_STEP * (3.75 / SPACING ** 2 + potential)
    divisor = 1.0 + diagonal * diagonal
    return jnp.stack([(vector[0] + diagonal * vector[1]) / divisor, (vector[1] - diagonal * vector[0]) / divisor])


def braket(left, right):
    real_part = jnp.sum(left[0] * right[0] + left[1] * right[1], axis=(1, 2, 3))
    imag_part = jnp.sum(left[0] * right[1] - left[1] * right[0], axis=(1, 2, 3))
    return real_part, imag_part


def times_complex(first, second):
    return (first[0] * second[0] - first[1] * second[1], first[0] * second[1] + first[1] * second[0])


def divide_complex(first, second):
    modulus = second[0] * second[0] + second[1] * second[1]
    return ((first[0] * second[0] + first[1] * second[1]) / modulus, (first[1] * second[0] - first[0] * second[1]) / modulus)


def scale_complex(coeff, vector):
    real_coef = coeff[0][:, None, None, None]
    imag_coef = coeff[1][:, None, None, None]
    return jnp.stack([real_coef * vector[0] - imag_coef * vector[1], real_coef * vector[1] + imag_coef * vector[0]])


def reference(orbitals, potential):
    h_orbitals = hamiltonian(orbitals, potential)
    residual = jnp.stack([2.0 * HALF_STEP * h_orbitals[1], -2.0 * HALF_STEP * h_orbitals[0]])
    evolved = orbitals
    shadow = residual
    direction = residual
    rho_now = braket(shadow, residual)
    for iteration in range(ITERS):
        dir_hat = precondition(direction, potential)
        image = system(dir_hat, hamiltonian(dir_hat, potential))
        alpha_step = divide_complex(rho_now, braket(shadow, image))
        half_step = residual - scale_complex(alpha_step, image)
        half_hat = precondition(half_step, potential)
        second = system(half_hat, hamiltonian(half_hat, potential))
        cross = braket(second, half_step)
        norm_second = jnp.sum(second * second, axis=(0, 2, 3, 4))
        omega_step = (cross[0] / norm_second, cross[1] / norm_second)
        evolved = evolved + scale_complex(alpha_step, dir_hat) + scale_complex(omega_step, half_hat)
        residual = half_step - scale_complex(omega_step, second)
        if iteration + 1 < ITERS:
            rho_next = braket(shadow, residual)
            beta_step = times_complex(divide_complex(rho_next, rho_now), divide_complex(alpha_step, omega_step))
            direction = residual + scale_complex(beta_step, direction - scale_complex(omega_step, image))
            rho_now = rho_next
    return evolved, residual
```

```python
import functools

import jax
import jax.numpy as jnp
from jax import lax
from jax.experimental import pallas as pl
from jax.experimental.pallas import tpu as pltpu
from jax.sharding import PartitionSpec as P

ITERS = 4
NB = 2 * ITERS + 1
SPACING = 0.25
HALF_STEP = 0.05
DIAG = 3.75 / SPACING**2
KAPPA = -0.5 / SPACING**2 * HALF_STEP * (4.0 / 3.0)
FAR = -1.0 / 16.0
MESH = pl.DeviceIdType.MESH
ROW = 8
IM = 64


def tri(i, j):
    return j * (j + 1) // 2 + i


def cmul(a, b):
    return (a[0] * b[0] - a[1] * b[1], a[0] * b[1] + a[1] * b[0])


def cconjmul(a, b):
    return (a[0] * b[0] + a[1] * b[1], a[0] * b[1] - a[1] * b[0])


def cdiv(a, b):
    modulus = b[0] * b[0] + b[1] * b[1]
    return ((a[0] * b[0] + a[1] * b[1]) / modulus, (a[1] * b[0] - a[0] * b[1]) / modulus)


def cadd(a, b):
    return (a[0] + b[0], a[1] + b[1])


def csub(a, b):
    return (a[0] - b[0], a[1] - b[1])


def csum(terms):
    while len(terms) > 1:
        terms = [cadd(terms[k], terms[k + 1]) if k + 1 < len(terms) else terms[k] for k in range(0, len(terms), 2)]
    return terms[0]


def shifted_sum(a):
    out = [a[0]]
    for k in range(1, len(a)):
        out.append(cadd(a[k], a[k - 1]))
    out.append(a[-1])
    return out


def axpy(a, s, b):
    out = []
    for k in range(max(len(a), len(b))):
        if k >= len(b):
            out.append(a[k])
        else:
            t = cmul(s, b[k])
            out.append(csub(a[k], t) if k < len(a) else (-t[0], -t[1]))
    return out


def recurrences(gram):
    def shadow_dot(a):
        return csum([cmul(gram(0, k), a[k]) for k in range(len(a))])

    one = jnp.ones_like(gram(0, 0)[0])
    zero = jnp.zeros_like(one)
    residual = [(one, zero)]
    direction = residual
    x = []
    rho = gram(0, 0)
    for iteration in range(ITERS):
        image = shifted_sum(direction)
        alpha = cdiv(rho, shadow_dot(image))
        half = axpy(residual, alpha, image)
        second = shifted_sum(half)
        n = len(second)
        g_second = [csum([cmul(gram(k, l), second[l]) for l in range(n)]) for k in range(n)]
        norm = csum([cconjmul(second[k], g_second[k]) for k in range(n)])[0]
        cross = csum([cconjmul(g_second[k], half[k]) for k in range(len(half))])
        omega = (cross[0] / norm, cross[1] / norm)
        minus = lambda s: (-s[0], -s[1])
        x = axpy(axpy(x, minus(alpha), direction), minus(omega), half)
        residual = axpy(half, omega, second)
        if iteration + 1 < ITERS:
            rho_next = shadow_dot(residual)
            beta = cmul(cdiv(rho_next, rho), cdiv(alpha, omega))
            direction = axpy(residual, minus(beta), axpy(direction, omega, image))
            rho = rho_next
    return residual, x


def kernel(
    nx, ny, orb_hbm, pot_ref, evolved_ref, residual_ref,
    u, w, pr, pi, gram, part_y, part_x, coef,
    load_sem, send_sem, recv_sem, ysend_sem, yrecv_sem, xsend_sem, xrecv_sem,
):
    norb, bx = orb_hbm.shape[1], orb_hbm.shape[2]
    io, ix, iy = lax.axis_index("orb"), lax.axis_index("gx"), lax.axis_index("gyz")
    rows = pl.ds(ROW, 8)

    loads = [
        pltpu.make_async_copy(orb_hbm.at[c, o], u.at[0, o, pl.ds(2, bx), c, rows], load_sem.at[o, c])
        for o in range(norb) for c in range(2)
    ]
    for copy in loads:
        copy.start()

    barrier = pltpu.get_barrier_semaphore()
    for d in range(1, ny):
        pl.semaphore_signal(barrier, inc=1, device_id=(io, ix, lax.rem(iy + d, ny)), device_id_type=MESH)
    for d in range(1, nx):
        pl.semaphore_signal(barrier, inc=1, device_id=(io, lax.rem(ix + d, nx), iy), device_id_type=MESH)

    everything = pl.ds(2, bx)
    sides = (
        (ix < nx - 1, (pl.ds(bx, 2), rows), (pl.ds(0, 2), rows), (io, ix + 1, iy), ix > 0),
        (ix > 0, (pl.ds(2, 2), rows), (pl.ds(bx + 2, 2), rows), (io, ix - 1, iy), ix < nx - 1),
        (iy < ny - 1, (everything, pl.ds(ROW + 6, 2)), (everything, pl.ds(ROW - 2, 2)), (io, ix, iy + 1), iy > 0),
        (iy > 0, (everything, pl.ds(ROW, 2)), (everything, pl.ds(ROW + 8, 2)), (io, ix, iy - 1), iy < ny - 1),
    )

    def halo(s, o, side):
        _, (sx, sr), (dx, dr), target, _ = sides[side]
        return pltpu.make_async_remote_copy(
            src_ref=u.at[s, o, sx, :, sr],
            dst_ref=u.at[s, o, dx, :, dr],
            send_sem=send_sem.at[s, o, side],
            recv_sem=recv_sem.at[s, o, side],
            device_id=target,
            device_id_type=MESH,
        )

    def send(s, o):
        for side in range(4):
            @pl.when(sides[side][0])
            def _():
                halo(s, o, side).start()

    def receive(s, o):
        for side in range(4):
            @pl.when(sides[side][4])
            def _():
                halo(s, o, side).wait_recv()

    def clear(side, _x, _r):
        @pl.when(jnp.logical_not(sides[side][4]))
        def _():
            def body(s, carry):
                for o in range(norb):
                    shape = (_x.size, 2, _r.size, 128)
                    u[s, o, _x, :, _r, :] = jnp.zeros(shape, jnp.float32)
                return carry
            lax.fori_loop(0, NB, body, 0)

    for side in range(4):
        clear(side, *sides[side][2])
    gram[...] = jnp.zeros_like(gram)

    def coefficients(x, carry):
        q = HALF_STEP * (DIAG + pot_ref[x])
        p = KAPPA / (1.0 + q * q)
        pr[x] = p
        pi[x] = -q * p
        return carry

    lax.fori_loop(0, bx, coefficients, 0, unroll=4)

    for copy in loads:
        copy.wait()
    pl.semaphore_wait(barrier, nx + ny - 2)
    for o in range(norb):
        send(0, o)

    lane = lax.broadcasted_iota(jnp.int32, (8, 128), 1)
    one, zero = jnp.float32(1.0), jnp.float32(0.0)
    near = (jnp.where(lane >= 1, one, zero), jnp.where(lane < 127, one, zero))
    far = (jnp.where(lane >= 2, FAR * one, zero), jnp.where(lane < 126, FAR * one, zero))

    def stencil(s, o, x, c):
        center = u[s, o, x + 2, c, rows]
        s1 = (u[s, o, x + 1, c, rows] + u[s, o, x + 3, c, rows]) + (
            u[s, o, x + 2, c, pl.ds(ROW - 1, 8)] + u[s, o, x + 2, c, pl.ds(ROW + 1, 8)]
        )
        s2 = (u[s, o, x, c, rows] + u[s, o, x + 4, c, rows]) + (
            u[s, o, x + 2, c, pl.ds(ROW - 2, 8)] + u[s, o, x + 2, c, pl.ds(ROW + 2, 8)]
        )
        z1 = near[0] * pltpu.roll(center, 1, 1) + near[1] * pltpu.roll(center, 127, 1)
        z2 = far[0] * pltpu.roll(center, 2, 1) + far[1] * pltpu.roll(center, 126, 1)
        return center, (s1 + z1) + (FAR * s2 + z2)

    def advance(s, o, first, last):
        def body(x, carry):
            c_re, t_re = stencil(s, o, x, 0)
            c_im, t_im = stencil(s, o, x, 1)
            if first:
                q = HALF_STEP * (DIAG + pot_ref[x])
                w_re = 2.0 * (KAPPA * t_im + q * c_im)
                w_im = -2.0 * (KAPPA * t_re + q * c_re)
            else:
                w_re, w_im = -t_im, t_re
            w[s, o, x, 0] = w_re
            w[s, o, x, 1] = w_im
            if not last:
                a, b = pr[x], pi[x]
                u[s + 1, o, x + 2, 0, rows] = a * w_re - b * w_im
                u[s + 1, o, x + 2, 1, rows] = a * w_im + b * w_re
            return carry
        lax.fori_loop(0, bx, body, 0, unroll=4)

    def products(s):
        def orbital(o, carry):
            def pair(i, carry):
                re, im = [], []
                for x in range(bx):
                    ar, ai, br, bi = w[i, o, x, 0], w[i, o, x, 1], w[s, o, x, 0], w[s, o, x, 1]
                    re.append(ar * br + ai * bi)
                    im.append(ar * bi - ai * br)
                row = s * (s + 1) // 2 + i
                for offset, terms in ((0, re), (IM, im)):
                    while len(terms) > 1:
                        terms = [terms[k] + terms[k + 1] for k in range(0, len(terms), 2)]
                    gram[o, pl.ds(offset + row, 1)] = jnp.sum(terms[0], axis=0, keepdims=True)
                return carry
            lax.fori_loop(0, s + 1, pair, 0)
            return carry
        lax.fori_loop(0, norb, orbital, 0)

    def step(s, first=False, last=False):
        for o in range(norb):
            receive(s, o)
            advance(s, o, first, last)
            if not last:
                send(s + 1, o)
        products(s)

    step(0, first=True)

    def middle(s, carry):
        step(s)
        return carry

    lax.fori_loop(1, NB - 1, middle, 0)
    step(NB - 1, last=True)

    ones = jnp.ones((8, 128), jnp.float32)
    row = lax.broadcasted_iota(jnp.int32, (8, 128), 0)
    mine = jnp.zeros((8, 128), jnp.float32)
    for o in range(norb):
        total = lax.dot_general(
            ones, gram[o], (((1,), (1,)), ((), ())),
            precision=lax.Precision.HIGHEST, preferred_element_type=jnp.float32,
        )
        mine = jnp.where(row == o, total, mine)

    def gather(part, me, n, target, ssem, rsem):
        def copy(d, slot):
            return pltpu.make_async_remote_copy(
                src_ref=part.at[me], dst_ref=part.at[slot],
                send_sem=ssem.at[d], recv_sem=rsem.at[slot],
                device_id=target(lax.rem(me + d, n)), device_id_type=MESH,
            )
        for d in range(1, n):
            copy(d, me).start()
        for d in range(1, n):
            copy(d, lax.rem(me + d, n)).wait_recv()
        for d in range(1, n):
            copy(d, me).wait_send()
        terms = [part[k] for k in range(n)]
        while len(terms) > 1:
            terms = [terms[k] + terms[k + 1] for k in range(0, len(terms), 2)]
        return terms[0]

    part_y[iy] = mine
    line = gather(part_y, iy, ny, lambda t: (io, ix, t), ysend_sem, yrecv_sem)
    part_x[ix] = line
    total = gather(part_x, ix, nx, lambda t: (io, t, iy), xsend_sem, xrecv_sem)

    def spread(e):
        return jnp.broadcast_to(total[:, e:e + 1], (8, 128))

    entries = {}
    for j in range(NB):
        for i in range(j + 1):
            re = spread(tri(i, j))
            im = jnp.zeros_like(re) if i == j else spread(IM + tri(i, j))
            entries[i, j] = (re, im)
            if i != j:
                entries[j, i] = (re, -im)
    res_coef, x_coef = recurrences(lambda i, j: entries[i, j])
    for k in range(NB):
        coef[0, k, 0], coef[0, k, 1] = res_coef[k]
        if k < NB - 1:
            coef[1, k, 0] = x_coef[k][0] * (1.0 / KAPPA)
            coef[1, k, 1] = x_coef[k][1] * (1.0 / KAPPA)

    for o in range(norb):
        def take(kind, k, c):
            return jnp.broadcast_to(coef[kind, k, c, pl.ds(o, 1)], (8, 128))

        rc = [(take(0, k, 0), take(0, k, 1)) for k in range(NB)]
        xc = [(take(1, k, 0), take(1, k, 1)) for k in range(NB - 1)]

        def combine(x, carry):
            vectors = [(w[k, o, x, 0], w[k, o, x, 1]) for k in range(NB)]
            res = csum([cmul(rc[k], vectors[k]) for k in range(NB)])
            inc = csum([cmul(xc[k], vectors[k]) for k in range(NB - 1)])
            inc = cmul((pr[x], pi[x]), inc)
            for c in range(2):
                residual_ref[c, o, x] = res[c]
                evolved_ref[c, o, x] = u[0, o, x + 2, c, rows] + inc[c]
            return carry

        lax.fori_loop(0, bx, combine, 0)

    def drain(s, carry):
        for o in range(norb):
            for side in range(4):
                @pl.when(sides[side][0])
                def _():
                    halo(s, o, side).wait_send()
        return carry

    lax.fori_loop(0, NB, drain, 0)


def solution(mesh):
    nx, ny = mesh.shape["gx"], mesh.shape["gyz"]

    def shards(orbitals, potential):
        _, norb, bx, by, nz = orbitals.shape
        block = jax.ShapeDtypeStruct(orbitals.shape, jnp.float32)
        return pl.pallas_call(
            functools.partial(kernel, nx, ny),
            out_shape=(block, block),
            in_specs=[pl.BlockSpec(memory_space=pl.ANY), pl.BlockSpec(memory_space=pltpu.VMEM)],
            out_specs=(pl.BlockSpec(memory_space=pltpu.VMEM), pl.BlockSpec(memory_space=pltpu.VMEM)),
            scratch_shapes=[
                pltpu.VMEM((NB, norb, bx + 4, 2, by + 16, nz), jnp.float32),
                pltpu.VMEM((NB, norb, bx, 2, by, nz), jnp.float32),
                pltpu.VMEM((bx, by, nz), jnp.float32),
                pltpu.VMEM((bx, by, nz), jnp.float32),
                pltpu.VMEM((norb, 128, 128), jnp.float32),
                pltpu.VMEM((ny, 8, 128), jnp.float32),
                pltpu.VMEM((nx, 8, 128), jnp.float32),
                pltpu.VMEM((2, NB, 2, 8, 128), jnp.float32),
                pltpu.SemaphoreType.DMA((norb, 2)),
                pltpu.SemaphoreType.DMA((NB, norb, 4)),
                pltpu.SemaphoreType.DMA((NB, norb, 4)),
                pltpu.SemaphoreType.DMA((ny,)),
                pltpu.SemaphoreType.DMA((ny,)),
                pltpu.SemaphoreType.DMA((nx,)),
                pltpu.SemaphoreType.DMA((nx,)),
            ],
            compiler_params=pltpu.CompilerParams(
                collective_id=0, has_side_effects=True, vmem_limit_bytes=48 * 2**20
            ),
        )(orbitals, potential)

    spec = P(None, "orb", "gx", "gyz", None)
    return jax.shard_map(
        shards, mesh=mesh, in_specs=(spec, P("gx", "gyz", None)), out_specs=(spec, spec), check_vma=False
    )
```

```python
import functools

import jax
import jax.numpy as jnp
from jax import lax
from jax.experimental import pallas as pl
from jax.experimental.pallas import tpu as pltpu
from jax.sharding import PartitionSpec as P

ITERS = 4
NB = 2 * ITERS + 1
SPACING = 0.25
HALF_STEP = 0.05
DIAG = 3.75 / SPACING**2
KAPPA = -0.5 / SPACING**2 * HALF_STEP * (4.0 / 3.0)
FAR = -1.0 / 16.0
MESH = pl.DeviceIdType.MESH
GROUP = 3
WIDTH = 2 * GROUP
NEAR = WIDTH - 2
ROW = 8
RC = 4
IM = 64


_ANGLE = (0.955336489, 0.295520207)
_NODES = (0.0, 0.6761480, -0.6761480, 0.0, 0.1811733, -0.1811733, 0.0, 0.4949747, -0.4949747)
SHIFT = tuple((t * _ANGLE[0], t * _ANGLE[1]) for t in _NODES)


def tri(i, j):
    return j * (j + 1) // 2 + i


def cmul(a, b):
    return (a[0] * b[0] - a[1] * b[1], a[0] * b[1] + a[1] * b[0])


def cconjmul(a, b):
    return (a[0] * b[0] + a[1] * b[1], a[0] * b[1] - a[1] * b[0])


def cdiv(a, b):
    modulus = b[0] * b[0] + b[1] * b[1]
    return ((a[0] * b[0] + a[1] * b[1]) / modulus, (a[1] * b[0] - a[0] * b[1]) / modulus)


def cadd(a, b):
    return (a[0] + b[0], a[1] + b[1])


def csub(a, b):
    return (a[0] - b[0], a[1] - b[1])


def csum(terms):
    while len(terms) > 1:
        terms = [cadd(terms[k], terms[k + 1]) if k + 1 < len(terms) else terms[k] for k in range(0, len(terms), 2)]
    return terms[0]


def shifted_sum(a):
    out = []
    for k in range(len(a)):
        re, im = SHIFT[k + 1]
        t = a[k] if re == 0.0 else cmul((1.0 + re, im), a[k])
        out.append(cadd(t, a[k - 1]) if k else t)
    out.append(a[-1])
    return out


def axpy(a, s, b):
    out = []
    for k in range(max(len(a), len(b))):
        if k >= len(b):
            out.append(a[k])
        else:
            t = cmul(s, b[k])
            out.append(csub(a[k], t) if k < len(a) else (-t[0], -t[1]))
    return out


def recurrences(gram):
    def shadow_dot(a):
        return csum([cmul(gram(0, k), a[k]) for k in range(len(a))])

    one = jnp.ones_like(gram(0, 0)[0])
    zero = jnp.zeros_like(one)
    residual = [(one, zero)]
    direction = residual
    x = []
    rho = gram(0, 0)
    for iteration in range(ITERS):
        image = shifted_sum(direction)
        alpha = cdiv(rho, shadow_dot(image))
        half = axpy(residual, alpha, image)
        second = shifted_sum(half)
        n = len(second)
        g_second = [csum([cmul(gram(k, l), second[l]) for l in range(n)]) for k in range(n)]
        norm = csum([cconjmul(second[k], g_second[k]) for k in range(n)])[0]
        cross = csum([cconjmul(g_second[k], half[k]) for k in range(len(half))])
        omega = (cross[0] / norm, cross[1] / norm)
        minus = lambda s: (-s[0], -s[1])
        x = axpy(axpy(x, minus(alpha), direction), minus(omega), half)
        residual = axpy(half, omega, second)
        if iteration + 1 < ITERS:
            rho_next = shadow_dot(residual)
            beta = cmul(cdiv(rho_next, rho), cdiv(alpha, omega))
            direction = axpy(residual, minus(beta), axpy(direction, omega, image))
            rho = rho_next
    return residual, x


def kernel(
    nx, ny, orb_hbm, pot_hbm, evolved_ref, residual_ref, *scratch,
):
    us, ws = scratch[:NB], scratch[NB:2 * NB]
    (pot, pr, pi, qf, gram, part_y, part_x, coef,
     load_sem, pot_sem, send_sem, recv_sem, ysend_sem, yrecv_sem, xsend_sem, xrecv_sem) = scratch[2 * NB:]
    norb, bx = orb_hbm.shape[1], orb_hbm.shape[2]
    io, ix, iy = lax.axis_index("orb"), lax.axis_index("gx"), lax.axis_index("gyz")
    rows = pl.ds(ROW, 8)

    loads = [pltpu.make_async_copy(pot_hbm, pot.at[pl.ds(NEAR, bx), rows], load_sem.at[2 * norb])] + [
        pltpu.make_async_copy(orb_hbm.at[c, o], us[0].at[o, pl.ds(WIDTH, bx), c, rows], load_sem.at[2 * o + c])
        for o in range(norb) for c in range(2)
    ]
    for copy in loads:
        copy.start()

    low_x, high_x, low_y, high_y = ix > 0, ix < nx - 1, iy > 0, iy < ny - 1
    exists = {-1: (low_x, low_y), 0: (None, None), 1: (high_x, high_y)}

    def present(dx, dy):
        a, b = exists[dx][0], exists[dy][1]
        return b if a is None else a if b is None else jnp.logical_and(a, b)

    sides = ((1, 0), (-1, 0), (0, 1), (0, -1), (1, 1), (1, -1), (-1, 1), (-1, -1))

    def span(d, length, first, width):
        if d == 0:
            return pl.ds(first, length), pl.ds(first, length)
        if d > 0:
            return pl.ds(first + length - width, width), pl.ds(first - width, width)
        return pl.ds(first, width), pl.ds(first + length, width)

    barrier = pltpu.get_barrier_semaphore()
    for d in range(1, ny):
        pl.semaphore_signal(barrier, inc=1, device_id=(io, ix, lax.rem(iy + d, ny)), device_id_type=MESH)
    for d in range(1, nx):
        pl.semaphore_signal(barrier, inc=1, device_id=(io, lax.rem(ix + d, nx), iy), device_id_type=MESH)
    expected = nx + ny - 2
    for dx, dy in sides[4:]:
        @pl.when(present(dx, dy))
        def _():
            pl.semaphore_signal(barrier, inc=1, device_id=(io, ix + dx, iy + dy), device_id_type=MESH)
        expected = expected + present(dx, dy).astype(jnp.int32)

    def pot_halo(side):
        dx, dy = sides[side]
        (sx, tx), (sr, tr) = span(dx, bx, NEAR, NEAR), span(dy, 8, ROW, NEAR)
        return pltpu.make_async_remote_copy(
            src_ref=pot.at[sx, sr], dst_ref=pot.at[tx, tr],
            send_sem=pot_sem.at[0, side], recv_sem=pot_sem.at[1, side],
            device_id=(io, ix + dx, iy + dy), device_id_type=MESH,
        )

    def halo(g, o, side):
        dx, dy = sides[side]
        width = NEAR if dx and dy else WIDTH
        (sx, tx), (sr, tr) = span(dx, bx, WIDTH, width), span(dy, 8, ROW, width)
        ref = us[GROUP * g]
        return pltpu.make_async_remote_copy(
            src_ref=ref.at[o, sx, :, sr], dst_ref=ref.at[o, tx, :, tr],
            send_sem=send_sem.at[g, o, side], recv_sem=recv_sem.at[g, o, side],
            device_id=(io, ix + dx, iy + dy), device_id_type=MESH,
        )

    def each_side(sent, act):
        for side, (dx, dy) in enumerate(sides):
            @pl.when(present(dx, dy) if sent else present(-dx, -dy))
            def _():
                act(side)

    def send(g, o):
        each_side(True, lambda side: halo(g, o, side).start())

    def receive(g, o):
        each_side(False, lambda side: halo(g, o, side).wait_recv())

    def clear(x0, nplanes, r0, nrows):
        def body(x, carry):
            for g in range(NB // GROUP):
                for o in range(norb):
                    us[GROUP * g][o, x, :, pl.ds(r0, nrows), :] = jnp.zeros((2, nrows, 128), jnp.float32)
            return carry
        lax.fori_loop(x0, x0 + nplanes, body, 0)

    def clear_pot(x0, nplanes, r0, nrows):
        pot[pl.ds(x0, nplanes), pl.ds(r0, nrows), :] = jnp.zeros((nplanes, nrows, 128), jnp.float32)

    for has, x0 in ((low_x, 0), (high_x, bx + WIDTH)):
        @pl.when(jnp.logical_not(has))
        def _():
            clear(x0, WIDTH, ROW - WIDTH, 8 + 2 * WIDTH)
            clear_pot(0 if x0 == 0 else bx + NEAR, NEAR, ROW - NEAR, 8 + 2 * NEAR)
    for has, r0 in ((low_y, ROW - WIDTH), (high_y, ROW + 8)):
        @pl.when(jnp.logical_not(has))
        def _():
            clear(0, bx + 2 * WIDTH, r0, WIDTH)
            clear_pot(0, bx + 2 * NEAR, ROW - NEAR if r0 < ROW else ROW + 8, NEAR)
    gram[...] = jnp.zeros_like(gram)

    for copy in loads:
        copy.wait()
    pl.semaphore_wait(barrier, expected)
    each_side(True, lambda side: pot_halo(side).start())
    for o in range(norb):
        send(0, o)

    zero, one = jnp.float32(0.0), jnp.float32(1.0)
    row = lax.broadcasted_iota(jnp.int32, (8, 128), 0)
    keep_rows = (
        jnp.where(jnp.logical_or(row >= ROW - RC, low_y), one, zero),
        jnp.where(jnp.logical_or(row < 8 - (ROW - RC), high_y), one, zero),
    )

    def coefficients(x, keep):
        for t in range(2):
            q = HALF_STEP * (DIAG + pot[x, pl.ds(RC + 8 * t, 8)])
            p = KAPPA / (1.0 + q * q) * keep_rows[t] * keep
            tile = pl.ds(8 * t, 8)
            qf[x, tile] = q
            pr[x, tile] = p
            pi[x, tile] = -q * p

    each_side(False, lambda side: pot_halo(side).wait_recv())
    lax.fori_loop(0, NEAR, lambda x, c: (coefficients(x, jnp.where(low_x, one, zero)), c)[1], 0)
    lax.fori_loop(NEAR, bx + NEAR, lambda x, c: (coefficients(x, one), c)[1], 0, unroll=4)
    lax.fori_loop(bx + NEAR, bx + 2 * NEAR, lambda x, c: (coefficients(x, jnp.where(high_x, one, zero)), c)[1], 0)

    lane = lax.broadcasted_iota(jnp.int32, (8, 128), 1)
    near = (jnp.where(lane >= 1, one, zero), jnp.where(lane < 127, one, zero))
    far = (jnp.where(lane >= 2, FAR * one, zero), jnp.where(lane < 126, FAR * one, zero))

    def stencil(u, o, x, c, r):
        def at(dx, dr):
            return u[o, x + WIDTH + dx, c, pl.ds(r + dr, 8)]
        center = at(0, 0)
        s1 = (at(-1, 0) + at(1, 0)) + (at(0, -1) + at(0, 1))
        s2 = (at(-2, 0) + at(2, 0)) + (at(0, -2) + at(0, 2))
        z1 = near[0] * pltpu.roll(center, 1, 1) + near[1] * pltpu.roll(center, 127, 1)
        z2 = far[0] * pltpu.roll(center, 2, 1) + far[1] * pltpu.roll(center, 126, 1)
        return center, (s1 + z1) + (FAR * s2 + z2)

    def wrows(s):
        return pl.ds(ROW - RC, 8) if s % GROUP < GROUP - 1 else pl.ds(0, 8)

    def advance(s, o):
        u, margin = us[s], WIDTH - 2 - 2 * (s % GROUP)
        a_shift, b_shift = SHIFT[s][0] / KAPPA, SHIFT[s][1] / KAPPA
        for x in range(-margin, bx + margin):
            out = -x if x < 0 else x - bx + 1 if x >= bx else 0
            beyond = margin - 2 * ((out + 1) // 2)
            for r in (ROW,) if beyond == 0 else (RC, RC + 8):
                u_re, t_re = stencil(u, o, x, 0, r)
                u_im, t_im = stencil(u, o, x, 1, r)
                tile = pl.ds(r - RC, 8)
                if s == 0:
                    q = qf[x + NEAR, tile]
                    w_re = 2.0 * (KAPPA * t_im + q * u_im)
                    w_im = -2.0 * (KAPPA * t_re + q * u_re)
                elif a_shift == 0.0:
                    w_re, w_im = -t_im, t_re
                else:
                    q = qf[x + NEAR, tile]
                    a, b = a_shift - b_shift * q, b_shift + a_shift * q
                    w_re = b * u_im - (t_im + a * u_re)
                    w_im = t_re - (a * u_im + b * u_re)
                if 0 <= x < bx:
                    dest = pl.ds(r - RC, 8) if beyond else pl.ds(0, 8)
                    ws[s][o, x, 0, dest] = w_re
                    ws[s][o, x, 1, dest] = w_im
                if s < NB - 1:
                    a, b = pr[x + NEAR, tile], pi[x + NEAR, tile]
                    us[s + 1][o, x + WIDTH, 0, pl.ds(r, 8)] = a * w_re - b * w_im
                    us[s + 1][o, x + WIDTH, 1, pl.ds(r, 8)] = a * w_im + b * w_re

    def vector(s, o, x):
        return ws[s][o, x, 0, wrows(s)], ws[s][o, x, 1, wrows(s)]

    def products(o, pairs):
        acc = {}
        used = sorted({k for pair in pairs for k in pair})
        for x in range(bx):
            v = {k: vector(k, o, x) for k in used}
            for i, j in pairs:
                (ar, ai), (br, bi) = v[i], v[j]
                terms = [ar * br + ai * bi] + ([ar * bi - ai * br] if i != j else [])
                for part, term in enumerate(terms):
                    key = (i, j, part, x % 2)
                    acc[key] = acc[key] + term if key in acc else term
        for i, j in pairs:
            for part in range(1 if i == j else 2):
                tile = acc[i, j, part, 0] + acc[i, j, part, 1]
                gram[o, pl.ds(part * IM + tri(i, j), 1)] = jnp.sum(tile, axis=0, keepdims=True)

    def column_products(g, o):
        new = range(GROUP * g, GROUP * g + GROUP)
        for i in range(GROUP * g):
            products(o, [(i, j) for j in new])
        products(o, [(i, j) for i in new for j in new if i <= j][:3])
        products(o, [(i, j) for i in new for j in new if i <= j][3:])

    groups = NB // GROUP
    for g in range(groups):
        def orbital(o, carry):
            receive(g, o)
            for s in range(GROUP * g, GROUP * g + GROUP):
                advance(s, o)
            if g < groups - 1:
                send(g + 1, o)
            else:
                column_products(g, o)
            return carry
        lax.fori_loop(0, norb, orbital, 0)
        if g < groups - 1:
            def gram_columns(o, carry):
                column_products(g, o)
                return carry
            lax.fori_loop(0, norb, gram_columns, 0)

    ones = jnp.ones((8, 128), jnp.float32)
    mine = jnp.zeros((8, 128), jnp.float32)
    for o in range(norb):
        total = lax.dot_general(
            ones, gram[o], (((1,), (1,)), ((), ())),
            precision=lax.Precision.HIGHEST, preferred_element_type=jnp.float32,
        )
        mine = jnp.where(row == o, total, mine)

    def gather(part, me, n, target, ssem, rsem):
        def copy(d, slot):
            return pltpu.make_async_remote_copy(
                src_ref=part.at[me], dst_ref=part.at[slot],
                send_sem=ssem.at[d], recv_sem=rsem.at[slot],
                device_id=target(lax.rem(me + d, n)), device_id_type=MESH,
            )
        for d in range(1, n):
            copy(d, me).start()
        for d in range(1, n):
            copy(d, lax.rem(me + d, n)).wait_recv()
        for d in range(1, n):
            copy(d, me).wait_send()
        terms = [part[k] for k in range(n)]
        while len(terms) > 1:
            terms = [terms[k] + terms[k + 1] for k in range(0, len(terms), 2)]
        return terms[0]

    part_y[iy] = mine
    line = gather(part_y, iy, ny, lambda t: (io, ix, t), ysend_sem, yrecv_sem)
    part_x[ix] = line
    total = gather(part_x, ix, nx, lambda t: (io, t, iy), xsend_sem, xrecv_sem)

    def spread(e):
        return jnp.broadcast_to(total[:, e:e + 1], (8, 128))

    entries = {}
    for j in range(NB):
        for i in range(j + 1):
            re = spread(tri(i, j))
            im = jnp.zeros_like(re) if i == j else spread(IM + tri(i, j))
            entries[i, j] = (re, im)
            if i != j:
                entries[j, i] = (re, -im)
    res_coef, x_coef = recurrences(lambda i, j: entries[i, j])
    for k in range(NB):
        coef[0, k, 0], coef[0, k, 1] = res_coef[k]
        if k < NB - 1:
            coef[1, k, 0] = x_coef[k][0] * (1.0 / KAPPA)
            coef[1, k, 1] = x_coef[k][1] * (1.0 / KAPPA)

    for o in range(norb):
        def take(kind, k, c):
            return jnp.broadcast_to(coef[kind, k, c, pl.ds(o, 1)], (8, 128))

        rc = [(take(0, k, 0), take(0, k, 1)) for k in range(NB)]
        xc = [(take(1, k, 0), take(1, k, 1)) for k in range(NB - 1)]

        def combine(x, carry):
            vectors = [vector(k, o, x) for k in range(NB)]
            res = csum([cmul(rc[k], vectors[k]) for k in range(NB)])
            inc = csum([cmul(xc[k], vectors[k]) for k in range(NB - 1)])
            inside = pl.ds(ROW - RC, 8)
            inc = cmul((pr[x + NEAR, inside], pi[x + NEAR, inside]), inc)
            for c in range(2):
                residual_ref[c, o, x] = res[c]
                evolved_ref[c, o, x] = us[0][o, x + WIDTH, c, rows] + inc[c]
            return carry

        lax.fori_loop(0, bx, combine, 0)

    each_side(True, lambda side: pot_halo(side).wait_send())
    for g in range(groups):
        def drain(o, carry):
            each_side(True, lambda side: halo(g, o, side).wait_send())
            return carry
        lax.fori_loop(0, norb, drain, 0)


def solution(mesh):
    nx, ny = mesh.shape["gx"], mesh.shape["gyz"]

    def shards(orbitals, potential):
        _, norb, bx, by, nz = orbitals.shape
        block = jax.ShapeDtypeStruct(orbitals.shape, jnp.float32)
        return pl.pallas_call(
            functools.partial(kernel, nx, ny),
            out_shape=(block, block),
            in_specs=[pl.BlockSpec(memory_space=pltpu.HBM)] * 2,
            out_specs=(pl.BlockSpec(memory_space=pltpu.VMEM), pl.BlockSpec(memory_space=pltpu.VMEM)),
            scratch_shapes=[
                pltpu.VMEM((norb, bx + 2 * WIDTH, 2, by + 16, nz), jnp.float32) for _ in range(NB)
            ] + [
                pltpu.VMEM((norb, bx, 2, 16 if s % GROUP < GROUP - 1 else 8, nz), jnp.float32) for s in range(NB)
            ] + [
                pltpu.VMEM((bx + 2 * NEAR, by + 16, nz), jnp.float32),
                pltpu.VMEM((bx + 2 * NEAR, 16, nz), jnp.float32),
                pltpu.VMEM((bx + 2 * NEAR, 16, nz), jnp.float32),
                pltpu.VMEM((bx + 2 * NEAR, 16, nz), jnp.float32),
                pltpu.VMEM((norb, 128, 128), jnp.float32),
                pltpu.VMEM((ny, 8, 128), jnp.float32),
                pltpu.VMEM((nx, 8, 128), jnp.float32),
                pltpu.VMEM((2, NB, 2, 8, 128), jnp.float32),
                pltpu.SemaphoreType.DMA((2 * norb + 1,)),
                pltpu.SemaphoreType.DMA((2, 8)),
                pltpu.SemaphoreType.DMA((NB // GROUP, norb, 8)),
                pltpu.SemaphoreType.DMA((NB // GROUP, norb, 8)),
                pltpu.SemaphoreType.DMA((ny,)),
                pltpu.SemaphoreType.DMA((ny,)),
                pltpu.SemaphoreType.DMA((nx,)),
                pltpu.SemaphoreType.DMA((nx,)),
            ],
            compiler_params=pltpu.CompilerParams(
                collective_id=0, has_side_effects=True, vmem_limit_bytes=48 * 2**20
            ),
        )(orbitals, potential)

    spec = P(None, "orb", "gx", "gyz", None)
    return jax.shard_map(
        shards, mesh=mesh, in_specs=(spec, P("gx", "gyz", None)), out_specs=(spec, spec), check_vma=False
    )
```

```python
import functools

import jax
import jax.numpy as jnp
from jax import lax
from jax.experimental import pallas as pl
from jax.experimental.pallas import tpu as pltpu
from jax.sharding import PartitionSpec as P

ITERS = 4
NB = 2 * ITERS + 1
SPACING = 0.25
HALF_STEP = 0.05
DIAG = 3.75 / SPACING**2
KAPPA = -0.5 / SPACING**2 * HALF_STEP * (4.0 / 3.0)
FAR = -1.0 / 16.0
MESH = pl.DeviceIdType.MESH
GROUP = 3
WIDTH = 2 * GROUP
NEAR = WIDTH - 2
ROW = 8
RC = 4
IM = 64


_ANGLE = (0.955336489, 0.295520207)
_NODES = (0.0, 0.6761480, -0.6761480, 0.0, 0.1811733, -0.1811733, 0.0, 0.4949747, -0.4949747)
SHIFT = tuple((t * _ANGLE[0], t * _ANGLE[1]) for t in _NODES)


def tri(i, j):
    return j * (j + 1) // 2 + i


def cmul(a, b):
    return (a[0] * b[0] - a[1] * b[1], a[0] * b[1] + a[1] * b[0])


def cconjmul(a, b):
    return (a[0] * b[0] + a[1] * b[1], a[0] * b[1] - a[1] * b[0])


def cdiv(a, b):
    modulus = b[0] * b[0] + b[1] * b[1]
    return ((a[0] * b[0] + a[1] * b[1]) / modulus, (a[1] * b[0] - a[0] * b[1]) / modulus)


def cadd(a, b):
    return (a[0] + b[0], a[1] + b[1])


def csub(a, b):
    return (a[0] - b[0], a[1] - b[1])


def csum(terms):
    while len(terms) > 1:
        terms = [cadd(terms[k], terms[k + 1]) if k + 1 < len(terms) else terms[k] for k in range(0, len(terms), 2)]
    return terms[0]


def shifted_sum(a):
    out = []
    for k in range(len(a)):
        re, im = SHIFT[k + 1]
        t = a[k] if re == 0.0 else cmul((1.0 + re, im), a[k])
        out.append(cadd(t, a[k - 1]) if k else t)
    out.append(a[-1])
    return out


def axpy(a, s, b):
    out = []
    for k in range(max(len(a), len(b))):
        if k >= len(b):
            out.append(a[k])
        else:
            t = cmul(s, b[k])
            out.append(csub(a[k], t) if k < len(a) else (-t[0], -t[1]))
    return out


def recurrences(gram):
    def shadow_dot(a):
        return csum([cmul(gram(0, k), a[k]) for k in range(len(a))])

    one = jnp.ones_like(gram(0, 0)[0])
    zero = jnp.zeros_like(one)
    residual = [(one, zero)]
    direction = residual
    x = []
    rho = gram(0, 0)
    for iteration in range(ITERS):
        image = shifted_sum(direction)
        alpha = cdiv(rho, shadow_dot(image))
        half = axpy(residual, alpha, image)
        second = shifted_sum(half)
        n = len(second)
        g_second = [csum([cmul(gram(k, l), second[l]) for l in range(n)]) for k in range(n)]
        norm = csum([cconjmul(second[k], g_second[k]) for k in range(n)])[0]
        cross = csum([cconjmul(g_second[k], half[k]) for k in range(len(half))])
        omega = (cross[0] / norm, cross[1] / norm)
        minus = lambda s: (-s[0], -s[1])
        x = axpy(axpy(x, minus(alpha), direction), minus(omega), half)
        residual = axpy(half, omega, second)
        if iteration + 1 < ITERS:
            rho_next = shadow_dot(residual)
            beta = cmul(cdiv(rho_next, rho), cdiv(alpha, omega))
            direction = axpy(residual, minus(beta), axpy(direction, omega, image))
            rho = rho_next
    return residual, x


def kernel(
    nx, ny, orb_hbm, pot_hbm, evolved_ref, residual_ref, *scratch,
):
    us, ws = scratch[:NB], scratch[NB:2 * NB]
    (pot, pr, pi, qf, gram, part_y, part_x, coef,
     ready, load_sem, pot_sem, send_sem, recv_sem, ysend_sem, yrecv_sem, xsend_sem, xrecv_sem) = scratch[2 * NB:]
    norb, bx = orb_hbm.shape[1], orb_hbm.shape[2]
    io, ix, iy = lax.axis_index("orb"), lax.axis_index("gx"), lax.axis_index("gyz")
    rows = pl.ds(ROW, 8)

    loads = [pltpu.make_async_copy(pot_hbm, pot.at[pl.ds(NEAR, bx), rows], load_sem.at[2 * norb])] + [
        pltpu.make_async_copy(orb_hbm.at[c, o], us[0].at[o, pl.ds(WIDTH, bx), c, rows], load_sem.at[2 * o + c])
        for o in range(norb) for c in range(2)
    ]
    for copy in loads:
        copy.start()

    low_x, high_x, low_y, high_y = ix > 0, ix < nx - 1, iy > 0, iy < ny - 1
    exists = {-1: (low_x, low_y), 0: (None, None), 1: (high_x, high_y)}

    def present(dx, dy):
        a, b = exists[dx][0], exists[dy][1]
        return b if a is None else a if b is None else jnp.logical_and(a, b)

    sides = ((1, 1), (1, -1), (-1, 1), (-1, -1), (1, 0), (-1, 0), (0, 1), (0, -1))

    def span(d, length, first, width):
        if d == 0:
            return pl.ds(first, length), pl.ds(first, length)
        if d > 0:
            return pl.ds(first + length - width, width), pl.ds(first - width, width)
        return pl.ds(first, width), pl.ds(first + length, width)

    def inside(dx, dy):
        ok = None
        for d, at, n in ((dx, ix, nx), (dy, iy, ny)):
            if d:
                here = at < n - d if d > 0 else at >= -d
                ok = here if ok is None else jnp.logical_and(ok, here)
        return ok

    def greet(sem, offsets):
        for dx, dy in offsets:
            @pl.when(inside(dx, dy))
            def _():
                pl.semaphore_signal(sem, inc=1, device_id=(io, ix + dx, iy + dy), device_id_type=MESH)

    def await_greetings(sem, offsets):
        pl.semaphore_wait(sem, sum(inside(dx, dy).astype(jnp.int32) for dx, dy in offsets))

    def around(dx, dy):
        return [(dx, 0), (-dx, 0), (0, dy), (0, -dy)]

    first = list(sides) + [(0, 2), (0, -2)]
    rounds = (around(1, 1) + [(0, 2), (0, -2)], around(2, 4), around(4, 8))
    assert nx <= 8 and ny <= 16
    barrier = pltpu.get_barrier_semaphore()
    greet(barrier, first)

    def pot_halo(side):
        dx, dy = sides[side]
        (sx, tx), (sr, tr) = span(dx, bx, NEAR, NEAR), span(dy, 8, ROW, NEAR)
        return pltpu.make_async_remote_copy(
            src_ref=pot.at[sx, sr], dst_ref=pot.at[tx, tr],
            send_sem=pot_sem.at[0, side], recv_sem=pot_sem.at[1, side],
            device_id=(io, ix + dx, iy + dy), device_id_type=MESH,
        )

    def halo(g, o, side):
        dx, dy = sides[side]
        width = NEAR if dx and dy else WIDTH
        (sx, tx), (sr, tr) = span(dx, bx, WIDTH, width), span(dy, 8, ROW, width)
        ref = us[GROUP * g]
        return pltpu.make_async_remote_copy(
            src_ref=ref.at[o, sx, :, sr], dst_ref=ref.at[o, tx, :, tr],
            send_sem=send_sem.at[g, o, side], recv_sem=recv_sem.at[g, o, side],
            device_id=(io, ix + dx, iy + dy), device_id_type=MESH,
        )

    def each_side(sent, act):
        for side, (dx, dy) in enumerate(sides):
            @pl.when(present(dx, dy) if sent else present(-dx, -dy))
            def _():
                act(side)

    def send(g, o):
        each_side(True, lambda side: halo(g, o, side).start())

    def receive(g, o):
        each_side(False, lambda side: halo(g, o, side).wait_recv())

    def clear(x0, nplanes, r0, nrows):
        def body(x, carry):
            for g in range(NB // GROUP):
                for o in range(norb):
                    us[GROUP * g][o, x, :, pl.ds(r0, nrows), :] = jnp.zeros((2, nrows, 128), jnp.float32)
            return carry
        lax.fori_loop(x0, x0 + nplanes, body, 0)

    def clear_pot(x0, nplanes, r0, nrows):
        pot[pl.ds(x0, nplanes), pl.ds(r0, nrows), :] = jnp.zeros((nplanes, nrows, 128), jnp.float32)

    for has, x0 in ((low_x, 0), (high_x, bx + WIDTH)):
        @pl.when(jnp.logical_not(has))
        def _():
            clear(x0, WIDTH, ROW - WIDTH, 8 + 2 * WIDTH)
            clear_pot(0 if x0 == 0 else bx + NEAR, NEAR, ROW - NEAR, 8 + 2 * NEAR)
    for has, r0 in ((low_y, ROW - WIDTH), (high_y, ROW + 8)):
        @pl.when(jnp.logical_not(has))
        def _():
            clear(0, bx + 2 * WIDTH, r0, WIDTH)
            clear_pot(0, bx + 2 * NEAR, ROW - NEAR if r0 < ROW else ROW + 8, NEAR)
    gram[...] = jnp.zeros_like(gram)

    for copy in loads:
        copy.wait()
    await_greetings(barrier, first)
    each_side(True, lambda side: pot_halo(side).start())
    for o in range(norb):
        send(0, o)
    greet(ready.at[0], rounds[0])

    zero, one = jnp.float32(0.0), jnp.float32(1.0)
    row = lax.broadcasted_iota(jnp.int32, (8, 128), 0)
    keep_rows = (
        jnp.where(jnp.logical_or(row >= ROW - RC, low_y), one, zero),
        jnp.where(jnp.logical_or(row < 8 - (ROW - RC), high_y), one, zero),
    )

    def coefficients(x, keep):
        for t in range(2):
            q = HALF_STEP * (DIAG + pot[x, pl.ds(RC + 8 * t, 8)])
            p = KAPPA / (1.0 + q * q) * keep_rows[t] * keep
            tile = pl.ds(8 * t, 8)
            qf[x, tile] = q
            pr[x, tile] = p
            pi[x, tile] = -q * p

    each_side(False, lambda side: pot_halo(side).wait_recv())
    lax.fori_loop(0, NEAR, lambda x, c: (coefficients(x, jnp.where(low_x, one, zero)), c)[1], 0)
    lax.fori_loop(NEAR, bx + NEAR, lambda x, c: (coefficients(x, one), c)[1], 0, unroll=4)
    lax.fori_loop(bx + NEAR, bx + 2 * NEAR, lambda x, c: (coefficients(x, jnp.where(high_x, one, zero)), c)[1], 0)

    lane = lax.broadcasted_iota(jnp.int32, (8, 128), 1)
    near = (jnp.where(lane >= 1, one, zero), jnp.where(lane < 127, one, zero))
    far = (jnp.where(lane >= 2, FAR * one, zero), jnp.where(lane < 126, FAR * one, zero))

    def stencil(u, o, x, c, r):
        def at(dx, dr):
            return u[o, x + WIDTH + dx, c, pl.ds(r + dr, 8)]
        center = at(0, 0)
        s1 = (at(-1, 0) + at(1, 0)) + (at(0, -1) + at(0, 1))
        s2 = (at(-2, 0) + at(2, 0)) + (at(0, -2) + at(0, 2))
        z1 = near[0] * pltpu.roll(center, 1, 1) + near[1] * pltpu.roll(center, 127, 1)
        z2 = far[0] * pltpu.roll(center, 2, 1) + far[1] * pltpu.roll(center, 126, 1)
        return center, (s1 + z1) + (FAR * s2 + z2)

    def wrows(s):
        return pl.ds(ROW - RC, 8) if s % GROUP < GROUP - 1 else pl.ds(0, 8)

    def advance(s, o):
        u, margin = us[s], WIDTH - 2 - 2 * (s % GROUP)
        a_shift, b_shift = SHIFT[s][0] / KAPPA, SHIFT[s][1] / KAPPA
        for x in range(-margin, bx + margin):
            out = -x if x < 0 else x - bx + 1 if x >= bx else 0
            beyond = margin - 2 * ((out + 1) // 2)
            for r in (ROW,) if beyond == 0 else (RC, RC + 8):
                u_re, t_re = stencil(u, o, x, 0, r)
                u_im, t_im = stencil(u, o, x, 1, r)
                tile = pl.ds(r - RC, 8)
                if s == 0:
                    q = qf[x + NEAR, tile]
                    w_re = 2.0 * (KAPPA * t_im + q * u_im)
                    w_im = -2.0 * (KAPPA * t_re + q * u_re)
                elif a_shift == 0.0:
                    w_re, w_im = -t_im, t_re
                else:
                    q = qf[x + NEAR, tile]
                    a, b = a_shift - b_shift * q, b_shift + a_shift * q
                    w_re = b * u_im - (t_im + a * u_re)
                    w_im = t_re - (a * u_im + b * u_re)
                if 0 <= x < bx:
                    dest = pl.ds(r - RC, 8) if beyond else pl.ds(0, 8)
                    ws[s][o, x, 0, dest] = w_re
                    ws[s][o, x, 1, dest] = w_im
                if s < NB - 1:
                    a, b = pr[x + NEAR, tile], pi[x + NEAR, tile]
                    us[s + 1][o, x + WIDTH, 0, pl.ds(r, 8)] = a * w_re - b * w_im
                    us[s + 1][o, x + WIDTH, 1, pl.ds(r, 8)] = a * w_im + b * w_re

    def vector(s, o, x):
        return ws[s][o, x, 0, wrows(s)], ws[s][o, x, 1, wrows(s)]

    def products(o, pairs):
        acc = {}
        used = sorted({k for pair in pairs for k in pair})
        for x in range(bx):
            v = {k: vector(k, o, x) for k in used}
            for i, j in pairs:
                (ar, ai), (br, bi) = v[i], v[j]
                terms = [ar * br + ai * bi] + ([ar * bi - ai * br] if i != j else [])
                for part, term in enumerate(terms):
                    key = (i, j, part, x % 2)
                    acc[key] = acc[key] + term if key in acc else term
        for i, j in pairs:
            for part in range(1 if i == j else 2):
                tile = acc[i, j, part, 0] + acc[i, j, part, 1]
                gram[o, pl.ds(part * IM + tri(i, j), 1)] = jnp.sum(tile, axis=0, keepdims=True)

    def column_products(g, o):
        new = range(GROUP * g, GROUP * g + GROUP)
        for i in range(GROUP * g):
            products(o, [(i, j) for j in new])
        products(o, [(i, j) for i in new for j in new if i <= j][:3])
        products(o, [(i, j) for i in new for j in new if i <= j][3:])

    groups = NB // GROUP
    for g in range(groups):
        def orbital(o, carry):
            receive(g, o)
            for s in range(GROUP * g, GROUP * g + GROUP):
                advance(s, o)
            if g < groups - 1:
                send(g + 1, o)
            else:
                column_products(g, o)
            return carry
        lax.fori_loop(0, norb, orbital, 0)
        await_greetings(ready.at[g], rounds[g])
        if g < groups - 1:
            greet(ready.at[g + 1], rounds[g + 1])

            def gram_columns(o, carry):
                column_products(g, o)
                return carry
            lax.fori_loop(0, norb, gram_columns, 0)

    ones = jnp.ones((8, 128), jnp.float32)
    mine = jnp.zeros((8, 128), jnp.float32)
    for o in range(norb):
        total = lax.dot_general(
            ones, gram[o], (((1,), (1,)), ((), ())),
            precision=lax.Precision.HIGHEST, preferred_element_type=jnp.float32,
        )
        mine = jnp.where(row == o, total, mine)

    def gather(part, me, n, target, ssem, rsem):
        def copy(d, slot):
            return pltpu.make_async_remote_copy(
                src_ref=part.at[me], dst_ref=part.at[slot],
                send_sem=ssem.at[d], recv_sem=rsem.at[slot],
                device_id=target(lax.rem(me + d, n)), device_id_type=MESH,
            )
        for d in range(1, n):
            copy(d, me).start()
        for d in range(1, n):
            copy(d, lax.rem(me + d, n)).wait_recv()
        for d in range(1, n):
            copy(d, me).wait_send()
        terms = [part[k] for k in range(n)]
        while len(terms) > 1:
            terms = [terms[k] + terms[k + 1] for k in range(0, len(terms), 2)]
        return terms[0]

    part_y[iy] = mine
    line = gather(part_y, iy, ny, lambda t: (io, ix, t), ysend_sem, yrecv_sem)
    part_x[ix] = line
    total = gather(part_x, ix, nx, lambda t: (io, t, iy), xsend_sem, xrecv_sem)

    def spread(e):
        return jnp.broadcast_to(total[:, e:e + 1], (8, 128))

    entries = {}
    for j in range(NB):
        for i in range(j + 1):
            re = spread(tri(i, j))
            im = jnp.zeros_like(re) if i == j else spread(IM + tri(i, j))
            entries[i, j] = (re, im)
            if i != j:
                entries[j, i] = (re, -im)
    res_coef, x_coef = recurrences(lambda i, j: entries[i, j])
    for k in range(NB):
        coef[0, k, 0], coef[0, k, 1] = res_coef[k]
        if k < NB - 1:
            coef[1, k, 0] = x_coef[k][0] * (1.0 / KAPPA)
            coef[1, k, 1] = x_coef[k][1] * (1.0 / KAPPA)

    for o in range(norb):
        def take(kind, k, c):
            return jnp.broadcast_to(coef[kind, k, c, pl.ds(o, 1)], (8, 128))

        rc = [(take(0, k, 0), take(0, k, 1)) for k in range(NB)]
        xc = [(take(1, k, 0), take(1, k, 1)) for k in range(NB - 1)]

        def combine(x, carry):
            vectors = [vector(k, o, x) for k in range(NB)]
            res = csum([cmul(rc[k], vectors[k]) for k in range(NB)])
            inc = csum([cmul(xc[k], vectors[k]) for k in range(NB - 1)])
            inside = pl.ds(ROW - RC, 8)
            inc = cmul((pr[x + NEAR, inside], pi[x + NEAR, inside]), inc)
            for c in range(2):
                residual_ref[c, o, x] = res[c]
                evolved_ref[c, o, x] = us[0][o, x + WIDTH, c, rows] + inc[c]
            return carry

        lax.fori_loop(0, bx, combine, 0)

    each_side(True, lambda side: pot_halo(side).wait_send())
    for g in range(groups):
        def drain(o, carry):
            each_side(True, lambda side: halo(g, o, side).wait_send())
            return carry
        lax.fori_loop(0, norb, drain, 0)


def solution(mesh):
    nx, ny = mesh.shape["gx"], mesh.shape["gyz"]

    def shards(orbitals, potential):
        _, norb, bx, by, nz = orbitals.shape
        block = jax.ShapeDtypeStruct(orbitals.shape, jnp.float32)
        return pl.pallas_call(
            functools.partial(kernel, nx, ny),
            out_shape=(block, block),
            in_specs=[pl.BlockSpec(memory_space=pltpu.HBM)] * 2,
            out_specs=(pl.BlockSpec(memory_space=pltpu.VMEM), pl.BlockSpec(memory_space=pltpu.VMEM)),
            scratch_shapes=[
                pltpu.VMEM((norb, bx + 2 * WIDTH, 2, by + 16, nz), jnp.float32) for _ in range(NB)
            ] + [
                pltpu.VMEM((norb, bx, 2, 16 if s % GROUP < GROUP - 1 else 8, nz), jnp.float32) for s in range(NB)
            ] + [
                pltpu.VMEM((bx + 2 * NEAR, by + 16, nz), jnp.float32),
                pltpu.VMEM((bx + 2 * NEAR, 16, nz), jnp.float32),
                pltpu.VMEM((bx + 2 * NEAR, 16, nz), jnp.float32),
                pltpu.VMEM((bx + 2 * NEAR, 16, nz), jnp.float32),
                pltpu.VMEM((norb, 128, 128), jnp.float32),
                pltpu.VMEM((ny, 8, 128), jnp.float32),
                pltpu.VMEM((nx, 8, 128), jnp.float32),
                pltpu.VMEM((2, NB, 2, 8, 128), jnp.float32),
                pltpu.SemaphoreType.REGULAR((NB // GROUP,)),
                pltpu.SemaphoreType.DMA((2 * norb + 1,)),
                pltpu.SemaphoreType.DMA((2, 8)),
                pltpu.SemaphoreType.DMA((NB // GROUP, norb, 8)),
                pltpu.SemaphoreType.DMA((NB // GROUP, norb, 8)),
                pltpu.SemaphoreType.DMA((ny,)),
                pltpu.SemaphoreType.DMA((ny,)),
                pltpu.SemaphoreType.DMA((nx,)),
                pltpu.SemaphoreType.DMA((nx,)),
            ],
            compiler_params=pltpu.CompilerParams(
                collective_id=0, has_side_effects=True, vmem_limit_bytes=48 * 2**20
            ),
        )(orbitals, potential)

    spec = P(None, "orb", "gx", "gyz", None)
    return jax.shard_map(
        shards, mesh=mesh, in_specs=(spec, P("gx", "gyz", None)), out_specs=(spec, spec), check_vma=False
    )
```

```python
import functools

import jax
import jax.numpy as jnp
from jax import lax
from jax.experimental import pallas as pl
from jax.experimental.pallas import tpu as pltpu
from jax.sharding import PartitionSpec as P

ITERS = 4
NB = 2 * ITERS + 1
SPACING = 0.25
HALF_STEP = 0.05
DIAG = 3.75 / SPACING**2
KAPPA = -0.5 / SPACING**2 * HALF_STEP * (4.0 / 3.0)
FAR = -1.0 / 16.0
MESH = pl.DeviceIdType.MESH
GROUP = 3
WIDTH = 2 * GROUP
NEAR = WIDTH - 2
ROW = 8
RC = 4
IM = 64


_ANGLE = (0.955336489, 0.295520207)
_NODES = (0.0, 0.6761480, -0.6761480, 0.0, 0.1811733, -0.1811733, 0.0, 0.4949747, -0.4949747)
SHIFT = tuple((t * _ANGLE[0], t * _ANGLE[1]) for t in _NODES)


def tri(i, j):
    return j * (j + 1) // 2 + i


def cmul(a, b):
    return (a[0] * b[0] - a[1] * b[1], a[0] * b[1] + a[1] * b[0])


def cconjmul(a, b):
    return (a[0] * b[0] + a[1] * b[1], a[0] * b[1] - a[1] * b[0])


def cdiv(a, b):
    modulus = b[0] * b[0] + b[1] * b[1]
    return ((a[0] * b[0] + a[1] * b[1]) / modulus, (a[1] * b[0] - a[0] * b[1]) / modulus)


def cadd(a, b):
    return (a[0] + b[0], a[1] + b[1])


def csub(a, b):
    return (a[0] - b[0], a[1] - b[1])


def csum(terms):
    while len(terms) > 1:
        terms = [cadd(terms[k], terms[k + 1]) if k + 1 < len(terms) else terms[k] for k in range(0, len(terms), 2)]
    return terms[0]


def shifted_sum(a):
    out = []
    for k in range(len(a)):
        re, im = SHIFT[k + 1]
        t = a[k] if re == 0.0 else cmul((1.0 + re, im), a[k])
        out.append(cadd(t, a[k - 1]) if k else t)
    out.append(a[-1])
    return out


def axpy(a, s, b):
    out = []
    for k in range(max(len(a), len(b))):
        if k >= len(b):
            out.append(a[k])
        else:
            t = cmul(s, b[k])
            out.append(csub(a[k], t) if k < len(a) else (-t[0], -t[1]))
    return out


def recurrences(gram):
    def shadow_dot(a):
        return csum([cmul(gram(0, k), a[k]) for k in range(len(a))])

    one = jnp.ones_like(gram(0, 0)[0])
    zero = jnp.zeros_like(one)
    residual = [(one, zero)]
    direction = residual
    x = []
    rho = gram(0, 0)
    for iteration in range(ITERS):
        image = shifted_sum(direction)
        alpha = cdiv(rho, shadow_dot(image))
        half = axpy(residual, alpha, image)
        second = shifted_sum(half)
        n = len(second)
        g_second = [csum([cmul(gram(k, l), second[l]) for l in range(n)]) for k in range(n)]
        norm = csum([cconjmul(second[k], g_second[k]) for k in range(n)])[0]
        cross = csum([cconjmul(g_second[k], half[k]) for k in range(len(half))])
        omega = (cross[0] / norm, cross[1] / norm)
        minus = lambda s: (-s[0], -s[1])
        x = axpy(axpy(x, minus(alpha), direction), minus(omega), half)
        residual = axpy(half, omega, second)
        if iteration + 1 < ITERS:
            rho_next = shadow_dot(residual)
            beta = cmul(cdiv(rho_next, rho), cdiv(alpha, omega))
            direction = axpy(residual, minus(beta), axpy(direction, omega, image))
            rho = rho_next
    return residual, x


def kernel(
    nx, ny, orb_hbm, pot_hbm, evolved_ref, residual_ref, *scratch,
):
    us = scratch[:NB + 1]
    (pot, pr, pi, qf, weight, gram, part_y, part_x,
     ready, load_sem, pot_sem, send_sem, recv_sem, ysend_sem, yrecv_sem, xsend_sem, xrecv_sem) = scratch[NB + 1:]
    norb, bx = orb_hbm.shape[1], orb_hbm.shape[2]
    io, ix, iy = lax.axis_index("orb"), lax.axis_index("gx"), lax.axis_index("gyz")
    rows = pl.ds(ROW, 8)

    loads = [pltpu.make_async_copy(pot_hbm, pot.at[pl.ds(NEAR, bx), rows], load_sem.at[2 * norb])] + [
        pltpu.make_async_copy(orb_hbm.at[c, o], us[0].at[o, pl.ds(WIDTH, bx), c, rows], load_sem.at[2 * o + c])
        for o in range(norb) for c in range(2)
    ]
    for copy in loads:
        copy.start()

    low_x, high_x, low_y, high_y = ix > 0, ix < nx - 1, iy > 0, iy < ny - 1
    exists = {-1: (low_x, low_y), 0: (None, None), 1: (high_x, high_y)}

    def present(dx, dy):
        a, b = exists[dx][0], exists[dy][1]
        return b if a is None else a if b is None else jnp.logical_and(a, b)

    sides = ((1, 1), (1, -1), (-1, 1), (-1, -1), (1, 0), (-1, 0), (0, 1), (0, -1))

    def span(d, length, first, width):
        if d == 0:
            return pl.ds(first, length), pl.ds(first, length)
        if d > 0:
            return pl.ds(first + length - width, width), pl.ds(first - width, width)
        return pl.ds(first, width), pl.ds(first + length, width)

    def inside(dx, dy):
        ok = None
        for d, at, n in ((dx, ix, nx), (dy, iy, ny)):
            if d:
                here = at < n - d if d > 0 else at >= -d
                ok = here if ok is None else jnp.logical_and(ok, here)
        return ok

    def greet(sem, offsets):
        for dx, dy in offsets:
            @pl.when(inside(dx, dy))
            def _():
                pl.semaphore_signal(sem, inc=1, device_id=(io, ix + dx, iy + dy), device_id_type=MESH)

    def await_greetings(sem, offsets):
        pl.semaphore_wait(sem, sum(inside(dx, dy).astype(jnp.int32) for dx, dy in offsets))

    def around(dx, dy):
        return [(dx, 0), (-dx, 0), (0, dy), (0, -dy)]

    first = list(sides) + [(0, 2), (0, -2)]
    rounds = (around(1, 1) + [(0, 2), (0, -2)], around(2, 4), around(4, 8))
    assert nx <= 8 and ny <= 16
    barrier = pltpu.get_barrier_semaphore()
    greet(barrier, first)

    def pot_halo(side):
        dx, dy = sides[side]
        (sx, tx), (sr, tr) = span(dx, bx, NEAR, NEAR), span(dy, 8, ROW, NEAR)
        return pltpu.make_async_remote_copy(
            src_ref=pot.at[sx, sr], dst_ref=pot.at[tx, tr],
            send_sem=pot_sem.at[0, side], recv_sem=pot_sem.at[1, side],
            device_id=(io, ix + dx, iy + dy), device_id_type=MESH,
        )

    def halo(g, o, side):
        dx, dy = sides[side]
        width = NEAR if dx and dy else WIDTH
        (sx, tx), (sr, tr) = span(dx, bx, WIDTH, width), span(dy, 8, ROW, width)
        ref = us[GROUP * g]
        return pltpu.make_async_remote_copy(
            src_ref=ref.at[o, sx, :, sr], dst_ref=ref.at[o, tx, :, tr],
            send_sem=send_sem.at[g, o, side], recv_sem=recv_sem.at[g, o, side],
            device_id=(io, ix + dx, iy + dy), device_id_type=MESH,
        )

    def each_side(sent, act):
        for side, (dx, dy) in enumerate(sides):
            @pl.when(present(dx, dy) if sent else present(-dx, -dy))
            def _():
                act(side)

    def send(g, o):
        each_side(True, lambda side: halo(g, o, side).start())

    def receive(g, o):
        each_side(False, lambda side: halo(g, o, side).wait_recv())

    def clear(x0, nplanes, r0, nrows):
        def body(x, carry):
            for g in range(NB // GROUP):
                for o in range(norb):
                    us[GROUP * g][o, x, :, pl.ds(r0, nrows), :] = jnp.zeros((2, nrows, 128), jnp.float32)
            return carry
        lax.fori_loop(x0, x0 + nplanes, body, 0)

    def clear_pot(x0, nplanes, r0, nrows):
        pot[pl.ds(x0, nplanes), pl.ds(r0, nrows), :] = jnp.zeros((nplanes, nrows, 128), jnp.float32)

    for has, x0 in ((low_x, 0), (high_x, bx + WIDTH)):
        @pl.when(jnp.logical_not(has))
        def _():
            clear(x0, WIDTH, ROW - WIDTH, 8 + 2 * WIDTH)
            clear_pot(0 if x0 == 0 else bx + NEAR, NEAR, ROW - NEAR, 8 + 2 * NEAR)
    for has, r0 in ((low_y, ROW - WIDTH), (high_y, ROW + 8)):
        @pl.when(jnp.logical_not(has))
        def _():
            clear(0, bx + 2 * WIDTH, r0, WIDTH)
            clear_pot(0, bx + 2 * NEAR, ROW - NEAR if r0 < ROW else ROW + 8, NEAR)
    gram[...] = jnp.zeros_like(gram)

    for copy in loads:
        copy.wait()
    await_greetings(barrier, first)
    each_side(True, lambda side: pot_halo(side).start())
    for o in range(norb):
        send(0, o)
    greet(ready.at[0], rounds[0])

    zero, one = jnp.float32(0.0), jnp.float32(1.0)
    row = lax.broadcasted_iota(jnp.int32, (8, 128), 0)
    keep_rows = (
        jnp.where(jnp.logical_or(row >= ROW - RC, low_y), one, zero),
        jnp.where(jnp.logical_or(row < 8 - (ROW - RC), high_y), one, zero),
    )

    def coefficients(x, keep):
        for t in range(2):
            q = HALF_STEP * (DIAG + pot[x, pl.ds(RC + 8 * t, 8)])
            p = KAPPA / (1.0 + q * q) * keep_rows[t] * keep
            tile = pl.ds(8 * t, 8)
            qf[x, tile] = q
            pr[x, tile] = p
            pi[x, tile] = -q * p

    def weights(x, carry):
        q = HALF_STEP * (DIAG + pot[x + NEAR, rows])
        weight[x] = (1.0 + q * q) * (1.0 / KAPPA**2)
        return carry

    lax.fori_loop(0, bx, weights, 0, unroll=4)
    await_greetings(ready.at[0], rounds[0])
    greet(ready.at[1], rounds[1])
    each_side(False, lambda side: pot_halo(side).wait_recv())
    lax.fori_loop(0, NEAR, lambda x, c: (coefficients(x, jnp.where(low_x, one, zero)), c)[1], 0)
    lax.fori_loop(NEAR, bx + NEAR, lambda x, c: (coefficients(x, one), c)[1], 0, unroll=4)
    lax.fori_loop(bx + NEAR, bx + 2 * NEAR, lambda x, c: (coefficients(x, jnp.where(high_x, one, zero)), c)[1], 0)

    lane = lax.broadcasted_iota(jnp.int32, (8, 128), 1)
    near = (jnp.where(lane >= 1, one, zero), jnp.where(lane < 127, one, zero))
    far = (jnp.where(lane >= 2, FAR * one, zero), jnp.where(lane < 126, FAR * one, zero))

    def stencil(u, o, x, c, r):
        def at(dx, dr):
            return u[o, x + WIDTH + dx, c, pl.ds(r + dr, 8)]
        center = at(0, 0)
        s1 = (at(-1, 0) + at(1, 0)) + (at(0, -1) + at(0, 1))
        s2 = (at(-2, 0) + at(2, 0)) + (at(0, -2) + at(0, 2))
        z1 = near[0] * pltpu.roll(center, 1, 1) + near[1] * pltpu.roll(center, 127, 1)
        z2 = far[0] * pltpu.roll(center, 2, 1) + far[1] * pltpu.roll(center, 126, 1)
        return center, (s1 + z1) + (FAR * s2 + z2)

    def advance(s, o):
        u, margin = us[s], WIDTH - 2 - 2 * (s % GROUP)
        for x in range(-margin, bx + margin):
            out = -x if x < 0 else x - bx + 1 if x >= bx else 0
            beyond = margin - 2 * ((out + 1) // 2)
            for r in (ROW,) if beyond == 0 else (RC, RC + 8):
                u_re, t_re = stencil(u, o, x, 0, r)
                u_im, t_im = stencil(u, o, x, 1, r)
                tile = pl.ds(r - RC, 8)
                a, b = pr[x + NEAR, tile], pi[x + NEAR, tile]
                if s == 0:
                    q = qf[x + NEAR, tile]
                    w_re = 2.0 * (KAPPA * t_im + q * u_im)
                    w_im = -2.0 * (KAPPA * t_re + q * u_re)
                    v_re, v_im = a * w_re - b * w_im, a * w_im + b * w_re
                else:
                    re, im = SHIFT[s]
                    v_re, v_im = -(a * t_im + b * t_re), a * t_re - b * t_im
                    if re != 0.0:
                        v_re = (im * u_im - a * t_im) - (re * u_re + b * t_re)
                        v_im = (a * t_re - re * u_im) - (im * u_re + b * t_im)
                us[s + 1][o, x + WIDTH, 0, pl.ds(r, 8)] = v_re
                us[s + 1][o, x + WIDTH, 1, pl.ds(r, 8)] = v_im

    def vector(k, o, x):
        return us[k + 1][o, x + WIDTH, 0, rows], us[k + 1][o, x + WIDTH, 1, rows]

    def products(o, pairs):
        acc = {}
        for x in range(bx):
            v = {k: vector(k, o, x) for k in sorted({k for pair in pairs for k in pair})}
            weighted = {i: (weight[x] * v[i][0], weight[x] * v[i][1]) for i in sorted({i for i, _ in pairs})}
            for i, j in pairs:
                (ar, ai), (br, bi) = weighted[i], v[j]
                terms = [ar * br + ai * bi] + ([ar * bi - ai * br] if i != j else [])
                for part, term in enumerate(terms):
                    key = (i, j, part, x % 2)
                    acc[key] = acc[key] + term if key in acc else term
        for i, j in pairs:
            for part in range(1 if i == j else 2):
                tile = acc[i, j, part, 0] + acc[i, j, part, 1]
                gram[o, pl.ds(part * IM + tri(i, j), 1)] = jnp.sum(tile, axis=0, keepdims=True)

    def column_products(g, o):
        new = range(GROUP * g, GROUP * g + GROUP)
        for i in range(GROUP * g):
            products(o, [(i, j) for j in new])
        products(o, [(i, j) for i in new for j in new if i <= j][:3])
        products(o, [(i, j) for i in new for j in new if i <= j][3:])

    def exchange(part, o, me, n, target, ssem, rsem):
        def copy(d, slot):
            return pltpu.make_async_remote_copy(
                src_ref=part.at[o, me], dst_ref=part.at[o, slot],
                send_sem=ssem.at[o, d], recv_sem=rsem.at[o, slot],
                device_id=target(lax.rem(me + d, n)), device_id_type=MESH,
            )
        order = sorted(range(1, n), key=lambda d: -min(d, n - d))

        def start(row):
            part[o, me] = row
            for d in order:
                copy(d, me).start()

        def total():
            for d in reversed(order):
                copy(d, lax.rem(me + d, n)).wait_recv()
            terms = [part[o, k] for k in range(n)]
            while len(terms) > 1:
                terms = [terms[k] + terms[k + 1] for k in range(0, len(terms), 2)]
            return terms[0]

        def drain():
            for d in order:
                copy(d, me).wait_send()

        return start, total, drain

    def over_y(o):
        return exchange(part_y, o, iy, ny, lambda t: (io, ix, t), ysend_sem, yrecv_sem)

    def over_x(o):
        return exchange(part_x, o, ix, nx, lambda t: (io, t, iy), xsend_sem, xrecv_sem)

    def start_reduction(o):
        sums = lax.dot_general(
            jnp.ones((8, 128), jnp.float32), gram[o], (((1,), (1,)), ((), ())),
            precision=lax.Precision.HIGHEST, preferred_element_type=jnp.float32,
        )
        over_y(o)[0](sums[0:1])

    groups = NB // GROUP
    for g in range(groups):
        def orbital(o, carry):
            receive(g, o)
            for s in range(GROUP * g, GROUP * g + GROUP):
                advance(s, o)
            if g < groups - 1:
                send(g + 1, o)
            else:
                column_products(g, o)
                start_reduction(o)
            return carry
        lax.fori_loop(0, norb, orbital, 0)
        if g == 0:
            await_greetings(ready.at[1], rounds[1])
            greet(ready.at[2], rounds[2])
        if g == 1:
            await_greetings(ready.at[2], rounds[2])
        if g < groups - 1:
            def gram_columns(o, carry):
                column_products(g, o)
                return carry
            lax.fori_loop(0, norb, gram_columns, 0)

    def second_stage(o, carry):
        over_x(o)[0](over_y(o)[1]())
        return carry

    lax.fori_loop(0, norb, second_stage, 0)

    each_side(True, lambda side: pot_halo(side).wait_send())
    for g in range(groups):
        def drain(o, carry):
            each_side(True, lambda side: halo(g, o, side).wait_send())
            return carry
        lax.fori_loop(0, norb, drain, 0)

    def drain_first(o, carry):
        over_y(o)[2]()
        return carry

    lax.fori_loop(0, norb, drain_first, 0)

    def finish(o, carry):
        total = jnp.broadcast_to(over_x(o)[1](), (8, 128))

        def spread(e):
            return jnp.broadcast_to(total[:, e:e + 1], (8, 128))

        entries = {}
        for j in range(NB):
            for i in range(j + 1):
                re = spread(tri(i, j))
                im = jnp.zeros_like(re) if i == j else spread(IM + tri(i, j))
                entries[i, j] = (re, im)
                if i != j:
                    entries[j, i] = (re, -im)
        res_coef, x_coef = recurrences(lambda i, j: entries[i, j])
        rc = [(c[0] * (1.0 / KAPPA), c[1] * (1.0 / KAPPA)) for c in res_coef]
        xc = [(c[0] * (1.0 / KAPPA), c[1] * (1.0 / KAPPA)) for c in x_coef]

        def combine(x, carry):
            vectors = [vector(k, o, x) for k in range(NB)]
            re, im = csum([cmul(rc[k], vectors[k]) for k in range(NB)])
            inc = csum([cmul(xc[k], vectors[k]) for k in range(NB - 1)])
            q = qf[x + NEAR, pl.ds(ROW - RC, 8)]
            residual_ref[0, o, x] = re - q * im
            residual_ref[1, o, x] = im + q * re
            for c in range(2):
                evolved_ref[c, o, x] = us[0][o, x + WIDTH, c, rows] + inc[c]
            return carry

        lax.fori_loop(0, bx, combine, 0, unroll=2)
        over_x(o)[2]()
        return carry

    lax.fori_loop(0, norb, finish, 0)


def solution(mesh):
    nx, ny = mesh.shape["gx"], mesh.shape["gyz"]

    def shards(orbitals, potential):
        _, norb, bx, by, nz = orbitals.shape
        block = jax.ShapeDtypeStruct(orbitals.shape, jnp.float32)
        return pl.pallas_call(
            functools.partial(kernel, nx, ny),
            out_shape=(block, block),
            in_specs=[pl.BlockSpec(memory_space=pltpu.HBM)] * 2,
            out_specs=(pl.BlockSpec(memory_space=pltpu.VMEM), pl.BlockSpec(memory_space=pltpu.VMEM)),
            scratch_shapes=[
                pltpu.VMEM((norb, bx + 2 * WIDTH, 2, by + 16, nz), jnp.float32) for _ in range(NB + 1)
            ] + [
                pltpu.VMEM((bx + 2 * NEAR, by + 16, nz), jnp.float32),
                pltpu.VMEM((bx + 2 * NEAR, 16, nz), jnp.float32),
                pltpu.VMEM((bx + 2 * NEAR, 16, nz), jnp.float32),
                pltpu.VMEM((bx + 2 * NEAR, 16, nz), jnp.float32),
                pltpu.VMEM((bx, by, nz), jnp.float32),
                pltpu.VMEM((norb, 128, 128), jnp.float32),
                pltpu.VMEM((norb, ny, 1, 128), jnp.float32),
                pltpu.VMEM((norb, nx, 1, 128), jnp.float32),
                pltpu.SemaphoreType.REGULAR((NB // GROUP,)),
                pltpu.SemaphoreType.DMA((2 * norb + 1,)),
                pltpu.SemaphoreType.DMA((2, 8)),
                pltpu.SemaphoreType.DMA((NB // GROUP, norb, 8)),
                pltpu.SemaphoreType.DMA((NB // GROUP, norb, 8)),
                pltpu.SemaphoreType.DMA((norb, ny)),
                pltpu.SemaphoreType.DMA((norb, ny)),
                pltpu.SemaphoreType.DMA((norb, nx)),
                pltpu.SemaphoreType.DMA((norb, nx)),
            ],
            compiler_params=pltpu.CompilerParams(
                collective_id=0, has_side_effects=True, vmem_limit_bytes=48 * 2**20
            ),
        )(*(pltpu.with_memory_space_constraint(a, pltpu.HBM) for a in (orbitals, potential)))

    spec = P(None, "orb", "gx", "gyz", None)
    return jax.shard_map(
        shards, mesh=mesh, in_specs=(spec, P("gx", "gyz", None)), out_specs=(spec, spec), check_vma=False
    )
```

```python
import functools

import jax
import jax.numpy as jnp
from jax import lax
from jax.experimental import pallas as pl
from jax.experimental.pallas import tpu as pltpu
from jax.sharding import PartitionSpec as P

ITERS = 4
NB = 2 * ITERS + 1
SPACING = 0.25
HALF_STEP = 0.05
DIAG = 3.75 / SPACING**2
KAPPA = -0.5 / SPACING**2 * HALF_STEP * (4.0 / 3.0)
FAR = -1.0 / 16.0
MESH = pl.DeviceIdType.MESH
GROUP = 3
WIDTH = 2 * GROUP
NEAR = WIDTH - 2
ROW = 8
RC = 4
IM = 64


_ANGLE = (0.955336489, 0.295520207)
_NODES = (0.0, 0.6761480, -0.6761480, 0.0, 0.1811733, -0.1811733, 0.0, 0.4949747, -0.4949747)
SHIFT = tuple((t * _ANGLE[0], t * _ANGLE[1]) for t in _NODES)


def tri(i, j):
    return j * (j + 1) // 2 + i


def cmul(a, b):
    return (a[0] * b[0] - a[1] * b[1], a[0] * b[1] + a[1] * b[0])


def cconjmul(a, b):
    return (a[0] * b[0] + a[1] * b[1], a[0] * b[1] - a[1] * b[0])


def cdiv(a, b):
    modulus = b[0] * b[0] + b[1] * b[1]
    return ((a[0] * b[0] + a[1] * b[1]) / modulus, (a[1] * b[0] - a[0] * b[1]) / modulus)


def cadd(a, b):
    return (a[0] + b[0], a[1] + b[1])


def csub(a, b):
    return (a[0] - b[0], a[1] - b[1])


def csum(terms):
    while len(terms) > 1:
        terms = [cadd(terms[k], terms[k + 1]) if k + 1 < len(terms) else terms[k] for k in range(0, len(terms), 2)]
    return terms[0]


def shifted_sum(a):
    out = []
    for k in range(len(a)):
        re, im = SHIFT[k + 1]
        t = a[k] if re == 0.0 else cmul((1.0 + re, im), a[k])
        out.append(cadd(t, a[k - 1]) if k else t)
    out.append(a[-1])
    return out


def axpy(a, s, b):
    out = []
    for k in range(max(len(a), len(b))):
        if k >= len(b):
            out.append(a[k])
        else:
            t = cmul(s, b[k])
            out.append(csub(a[k], t) if k < len(a) else (-t[0], -t[1]))
    return out


def recurrences(gram):
    def shadow_dot(a):
        return csum([cmul(gram(0, k), a[k]) for k in range(len(a))])

    one = jnp.ones_like(gram(0, 0)[0])
    zero = jnp.zeros_like(one)
    residual = [(one, zero)]
    direction = residual
    x = []
    rho = gram(0, 0)
    for iteration in range(ITERS):
        image = shifted_sum(direction)
        alpha = cdiv(rho, shadow_dot(image))
        half = axpy(residual, alpha, image)
        second = shifted_sum(half)
        n = len(second)
        g_second = [csum([cmul(gram(k, l), second[l]) for l in range(n)]) for k in range(n)]
        norm = csum([cconjmul(second[k], g_second[k]) for k in range(n)])[0]
        cross = csum([cconjmul(g_second[k], half[k]) for k in range(len(half))])
        omega = (cross[0] / norm, cross[1] / norm)
        minus = lambda s: (-s[0], -s[1])
        x = axpy(axpy(x, minus(alpha), direction), minus(omega), half)
        residual = axpy(half, omega, second)
        if iteration + 1 < ITERS:
            rho_next = shadow_dot(residual)
            beta = cmul(cdiv(rho_next, rho), cdiv(alpha, omega))
            direction = axpy(residual, minus(beta), axpy(direction, omega, image))
            rho = rho_next
    return residual, x


def kernel(
    nx, ny, orb_hbm, pot_hbm, evolved_ref, residual_ref, *scratch,
):
    (ux, *us) = scratch[:NB + 2 - NB // GROUP]
    us = [ux.at[k // GROUP] if k % GROUP == 0 and k < NB else us.pop(0) for k in range(NB + 1)]
    (pot, ballast, pr, pi, qf, weight, gram, part_y, part_x,
     ready, load_sem, pot_sem, send_sem, recv_sem, ysend_sem, yrecv_sem, xsend_sem, xrecv_sem) = scratch[NB + 2 - NB // GROUP:]
    norb, bx = orb_hbm.shape[1], orb_hbm.shape[2]
    io, ix, iy = lax.axis_index("orb"), lax.axis_index("gx"), lax.axis_index("gyz")
    rows = pl.ds(ROW, 8)

    load_pot = pltpu.make_async_copy(pot_hbm, pot.at[pl.ds(NEAR, bx), rows], load_sem.at[0])
    load_pot.start()
    for o in range(norb):
        for c in range(2):
            pltpu.make_async_copy(
                orb_hbm.at[c, o], us[0].at[o, pl.ds(WIDTH, bx), c, rows], load_sem.at[1]
            ).start()

    low_x, high_x, low_y, high_y = ix > 0, ix < nx - 1, iy > 0, iy < ny - 1
    exists = {-1: (low_x, low_y), 0: (None, None), 1: (high_x, high_y)}

    def present(dx, dy):
        a, b = exists[dx][0], exists[dy][1]
        return b if a is None else a if b is None else jnp.logical_and(a, b)

    sides = ((1, 1), (1, -1), (-1, 1), (-1, -1), (1, 0), (-1, 0), (0, 1), (0, -1))

    def span(d, length, first, width):
        if d == 0:
            return pl.ds(first, length), pl.ds(first, length)
        if d > 0:
            return pl.ds(first + length - width, width), pl.ds(first - width, width)
        return pl.ds(first, width), pl.ds(first + length, width)

    def inside(dx, dy):
        ok = None
        for d, at, n in ((dx, ix, nx), (dy, iy, ny)):
            if d:
                here = at < n - d if d > 0 else at >= -d
                ok = here if ok is None else jnp.logical_and(ok, here)
        return ok

    def greet(sem, offsets):
        for dx, dy in offsets:
            @pl.when(inside(dx, dy))
            def _():
                pl.semaphore_signal(sem, inc=1, device_id=(io, ix + dx, iy + dy), device_id_type=MESH)

    def await_greetings(sem, offsets):
        pl.semaphore_wait(sem, sum(inside(dx, dy).astype(jnp.int32) for dx, dy in offsets))

    def around(dx, dy):
        return [(dx, 0), (-dx, 0), (0, dy), (0, -dy)]

    first = list(sides) + [(0, 2), (0, -2)]
    rounds = (around(1, 1) + [(0, 2), (0, -2)], around(2, 4), around(4, 8))
    assert nx <= 8 and ny <= 16
    barrier = pltpu.get_barrier_semaphore()
    greet(barrier, first)

    def pot_halo(side):
        dx, dy = sides[side]
        (sx, tx), (sr, tr) = span(dx, bx, NEAR, NEAR), span(dy, 8, ROW, NEAR)
        return pltpu.make_async_remote_copy(
            src_ref=pot.at[sx, sr], dst_ref=pot.at[tx, tr],
            send_sem=pot_sem.at[0], recv_sem=pot_sem.at[1],
            device_id=(io, ix + dx, iy + dy), device_id_type=MESH,
        )

    def halo_spans(side):
        dx, dy = sides[side]
        width = NEAR if dx and dy else WIDTH
        return span(dx, bx, WIDTH, width), span(dy, 8, ROW, width)

    def halo(g, o, side):
        dx, dy = sides[side]
        (sx, tx), (sr, tr) = halo_spans(side)
        ref = us[GROUP * g]
        return pltpu.make_async_remote_copy(
            src_ref=ref.at[o, sx, :, sr], dst_ref=ref.at[o, tx, :, tr],
            send_sem=send_sem.at[side], recv_sem=recv_sem.at[g % 2, o],
            device_id=(io, ix + dx, iy + dy), device_id_type=MESH,
        )

    def each_side(act):
        for side, (dx, dy) in enumerate(sides):
            @pl.when(present(dx, dy))
            def _():
                act(side)

    def send(g, o):
        each_side(lambda side: halo(g, o, side).start())

    both_x, both_y = jnp.logical_and(low_x, high_x), jnp.logical_and(low_y, high_y)

    def await_sides(sem, planes, wide, corner):
        for nsx in (1, 2):
            for nsy in (1, 2):
                here = jnp.logical_and(both_x if nsx == 2 else jnp.logical_not(both_x),
                                       both_y if nsy == 2 else jnp.logical_not(both_y))
                total = planes * (nsx * wide * 8 + nsy * bx * wide + nsx * nsy * corner * corner)
                ref = ballast.at[pl.ds(0, total)]

                @pl.when(here)
                def _():
                    pltpu.make_async_copy(ref, ref, sem).wait()

    def receive(g, o):
        await_sides(recv_sem.at[g % 2, o], 2, WIDTH, NEAR)

    def clear(x0, nplanes, r0, nrows):
        def body(x, carry):
            for g in range(NB // GROUP):
                for o in range(norb):
                    us[GROUP * g][o, x, :, pl.ds(r0, nrows), :] = jnp.zeros((2, nrows, 128), jnp.float32)
            return carry
        lax.fori_loop(x0, x0 + nplanes, body, 0)

    def clear_pot(x0, nplanes, r0, nrows):
        pot[pl.ds(x0, nplanes), pl.ds(r0, nrows), :] = jnp.zeros((nplanes, nrows, 128), jnp.float32)

    for has, x0 in ((low_x, 0), (high_x, bx + WIDTH)):
        @pl.when(jnp.logical_not(has))
        def _():
            clear(x0, WIDTH, ROW - WIDTH, 8 + 2 * WIDTH)
            clear_pot(0 if x0 == 0 else bx + NEAR, NEAR, ROW - NEAR, 8 + 2 * NEAR)
    for has, r0 in ((low_y, ROW - WIDTH), (high_y, ROW + 8)):
        @pl.when(jnp.logical_not(has))
        def _():
            clear(0, bx + 2 * WIDTH, r0, WIDTH)
            clear_pot(0, bx + 2 * NEAR, ROW - NEAR if r0 < ROW else ROW + 8, NEAR)
    gram[...] = jnp.zeros_like(gram)

    block = us[0].at[:, pl.ds(WIDTH, bx), :, rows]
    load_pot.wait()
    pltpu.make_async_copy(block, block, load_sem.at[1]).wait()
    await_greetings(barrier, first)
    each_side(lambda side: pot_halo(side).start())
    for o in range(norb):
        send(0, o)
    greet(ready.at[0], rounds[0])

    zero, one = jnp.float32(0.0), jnp.float32(1.0)
    row = lax.broadcasted_iota(jnp.int32, (8, 128), 0)
    keep_rows = (
        jnp.where(jnp.logical_or(row >= ROW - RC, low_y), one, zero),
        jnp.where(jnp.logical_or(row < 8 - (ROW - RC), high_y), one, zero),
    )

    def coefficients(x, keep):
        for t in range(2):
            q = HALF_STEP * (DIAG + pot[x, pl.ds(RC + 8 * t, 8)])
            p = KAPPA / (1.0 + q * q) * keep_rows[t] * keep
            tile = pl.ds(8 * t, 8)
            qf[x, tile] = q
            pr[x, tile] = p
            pi[x, tile] = -q * p

    def weights(x, carry):
        q = HALF_STEP * (DIAG + pot[x + NEAR, rows])
        weight[x] = (1.0 + q * q) * (1.0 / KAPPA**2)
        return carry

    lax.fori_loop(0, bx, weights, 0, unroll=4)
    await_greetings(ready.at[0], rounds[0])
    greet(ready.at[1], rounds[1])
    await_sides(pot_sem.at[1], 1, NEAR, NEAR)
    lax.fori_loop(0, NEAR, lambda x, c: (coefficients(x, jnp.where(low_x, one, zero)), c)[1], 0)
    lax.fori_loop(NEAR, bx + NEAR, lambda x, c: (coefficients(x, one), c)[1], 0, unroll=4)
    lax.fori_loop(bx + NEAR, bx + 2 * NEAR, lambda x, c: (coefficients(x, jnp.where(high_x, one, zero)), c)[1], 0)

    lane = lax.broadcasted_iota(jnp.int32, (8, 128), 1)
    near = (jnp.where(lane >= 1, one, zero), jnp.where(lane < 127, one, zero))
    far = (jnp.where(lane >= 2, FAR * one, zero), jnp.where(lane < 126, FAR * one, zero))

    def stencil(u, o, x, c, r):
        def at(dx, dr):
            return u[o, x + WIDTH + dx, c, pl.ds(r + dr, 8)]
        center = at(0, 0)
        s1 = (at(-1, 0) + at(1, 0)) + (at(0, -1) + at(0, 1))
        s2 = (at(-2, 0) + at(2, 0)) + (at(0, -2) + at(0, 2))
        z1 = near[0] * pltpu.roll(center, 1, 1) + near[1] * pltpu.roll(center, 127, 1)
        z2 = far[0] * pltpu.roll(center, 2, 1) + far[1] * pltpu.roll(center, 126, 1)
        return center, (s1 + z1) + (FAR * s2 + z2)

    def advance(s, o):
        u, margin = us[s], WIDTH - 2 - 2 * (s % GROUP)
        for x in range(-margin, bx + margin):
            out = -x if x < 0 else x - bx + 1 if x >= bx else 0
            beyond = margin - 2 * ((out + 1) // 2)
            for r in (ROW,) if beyond == 0 else (RC, RC + 8):
                u_re, t_re = stencil(u, o, x, 0, r)
                u_im, t_im = stencil(u, o, x, 1, r)
                tile = pl.ds(r - RC, 8)
                a, b = pr[x + NEAR, tile], pi[x + NEAR, tile]
                if s == 0:
                    q = qf[x + NEAR, tile]
                    w_re = 2.0 * (KAPPA * t_im + q * u_im)
                    w_im = -2.0 * (KAPPA * t_re + q * u_re)
                    v_re, v_im = a * w_re - b * w_im, a * w_im + b * w_re
                else:
                    re, im = SHIFT[s]
                    v_re, v_im = -(a * t_im + b * t_re), a * t_re - b * t_im
                    if re != 0.0:
                        v_re = (im * u_im - a * t_im) - (re * u_re + b * t_re)
                        v_im = (a * t_re - re * u_im) - (im * u_re + b * t_im)
                us[s + 1][o, x + WIDTH, 0, pl.ds(r, 8)] = v_re
                us[s + 1][o, x + WIDTH, 1, pl.ds(r, 8)] = v_im

    def vector(k, o, x):
        return us[k + 1][o, x + WIDTH, 0, rows], us[k + 1][o, x + WIDTH, 1, rows]

    def products(o, pairs):
        acc = {}
        for x in range(bx):
            v = {k: vector(k, o, x) for k in sorted({k for pair in pairs for k in pair})}
            weighted = {i: (weight[x] * v[i][0], weight[x] * v[i][1]) for i in sorted({i for i, _ in pairs})}
            for i, j in pairs:
                (ar, ai), (br, bi) = weighted[i], v[j]
                terms = [ar * br + ai * bi] + ([ar * bi - ai * br] if i != j else [])
                for part, term in enumerate(terms):
                    key = (i, j, part, x % 2)
                    acc[key] = acc[key] + term if key in acc else term
        for i, j in pairs:
            for part in range(1 if i == j else 2):
                tile = acc[i, j, part, 0] + acc[i, j, part, 1]
                gram[o, pl.ds(part * IM + tri(i, j), 1)] = jnp.sum(tile, axis=0, keepdims=True)

    def column_products(g, o):
        new = range(GROUP * g, GROUP * g + GROUP)
        for i in range(GROUP * g):
            products(o, [(i, j) for j in new])
        products(o, [(i, j) for i in new for j in new if i <= j][:3])
        products(o, [(i, j) for i in new for j in new if i <= j][3:])

    def exchange(part, me, n, target, ssem, rsem):
        def start(o, row):
            part[o, me] = row
            for d in sorted(range(1, n), key=lambda d: -min(d, n - d)):
                pltpu.make_async_remote_copy(
                    src_ref=part.at[o, me], dst_ref=part.at[o, me], send_sem=ssem, recv_sem=rsem.at[o],
                    device_id=target(lax.rem(me + d, n)), device_id_type=MESH,
                ).start()

        def total(o):
            others = part.at[o, pl.ds(0, n - 1)]
            pltpu.make_async_copy(others, others, rsem.at[o]).wait()
            terms = [part[o, k] for k in range(n)]
            while len(terms) > 1:
                terms = [terms[k] + terms[k + 1] for k in range(0, len(terms), 2)]
            return terms[0]

        def drain():
            others = part.at[:, pl.ds(0, n - 1)]
            pltpu.make_async_copy(others, others, ssem).wait()

        return start, total, drain

    start_y, total_y, drain_y = exchange(part_y, iy, ny, lambda t: (io, ix, t), ysend_sem.at[0], yrecv_sem)
    start_x, total_x, drain_x = exchange(part_x, ix, nx, lambda t: (io, t, iy), xsend_sem.at[0], xrecv_sem)

    def start_reduction(o):
        sums = lax.dot_general(
            jnp.ones((8, 128), jnp.float32), gram[o], (((1,), (1,)), ((), ())),
            precision=lax.Precision.HIGHEST, preferred_element_type=jnp.float32,
        )
        start_y(o, sums[0:1])

    groups = NB // GROUP
    for g in range(groups):
        def orbital(o, carry):
            receive(g, o)
            for s in range(GROUP * g, GROUP * g + GROUP):
                advance(s, o)
            if g < groups - 1:
                send(g + 1, o)
            else:
                column_products(g, o)
                start_reduction(o)
            return carry
        lax.fori_loop(0, norb, orbital, 0)
        if g == 0:
            await_greetings(ready.at[1], rounds[1])
            greet(ready.at[2], rounds[2])
        if g == 1:
            await_greetings(ready.at[2], rounds[2])
        if g < groups - 1:
            def gram_columns(o, carry):
                column_products(g, o)
                return carry
            lax.fori_loop(0, norb, gram_columns, 0)

    def second_stage(o, carry):
        start_x(o, total_y(o))
        return carry

    lax.fori_loop(0, norb, second_stage, 0)

    await_sides(pot_sem.at[0], 1, NEAR, NEAR)
    for side, (dx, dy) in enumerate(sides):
        (sx, _), (sr, _) = halo_spans(side)
        sent = ux.at[:, :, sx, :, sr]

        @pl.when(present(dx, dy))
        def _():
            pltpu.make_async_copy(sent, sent, send_sem.at[side]).wait()
    drain_y()

    def finish(o, carry):
        total = jnp.broadcast_to(total_x(o), (8, 128))

        def spread(e):
            return jnp.broadcast_to(total[:, e:e + 1], (8, 128))

        entries = {}
        for j in range(NB):
            for i in range(j + 1):
                re = spread(tri(i, j))
                im = jnp.zeros_like(re) if i == j else spread(IM + tri(i, j))
                entries[i, j] = (re, im)
                if i != j:
                    entries[j, i] = (re, -im)
        res_coef, x_coef = recurrences(lambda i, j: entries[i, j])
        rc = [(c[0] * (1.0 / KAPPA), c[1] * (1.0 / KAPPA)) for c in res_coef]
        xc = [(c[0] * (1.0 / KAPPA), c[1] * (1.0 / KAPPA)) for c in x_coef]

        def combine(x, carry):
            vectors = [vector(k, o, x) for k in range(NB)]
            re, im = csum([cmul(rc[k], vectors[k]) for k in range(NB)])
            inc = csum([cmul(xc[k], vectors[k]) for k in range(NB - 1)])
            q = qf[x + NEAR, pl.ds(ROW - RC, 8)]
            residual_ref[0, o, x] = re - q * im
            residual_ref[1, o, x] = im + q * re
            for c in range(2):
                evolved_ref[c, o, x] = us[0][o, x + WIDTH, c, rows] + inc[c]
            return carry

        lax.fori_loop(0, bx, combine, 0, unroll=2)
        return carry

    lax.fori_loop(0, norb, finish, 0)
    drain_x()


def solution(mesh):
    nx, ny = mesh.shape["gx"], mesh.shape["gyz"]

    def shards(orbitals, potential):
        _, norb, bx, by, nz = orbitals.shape
        block = jax.ShapeDtypeStruct(orbitals.shape, jnp.float32)
        return pl.pallas_call(
            functools.partial(kernel, nx, ny),
            out_shape=(block, block),
            in_specs=[pl.BlockSpec(memory_space=pltpu.HBM)] * 2,
            out_specs=(pl.BlockSpec(memory_space=pltpu.VMEM), pl.BlockSpec(memory_space=pltpu.VMEM)),
            scratch_shapes=[
                pltpu.VMEM((NB // GROUP, norb, bx + 2 * WIDTH, 2, by + 16, nz), jnp.float32)
            ] + [
                pltpu.VMEM((norb, bx + 2 * WIDTH, 2, by + 16, nz), jnp.float32) for _ in range(NB + 1 - NB // GROUP)
            ] + [
                pltpu.VMEM((bx + 2 * NEAR, by + 16, nz), jnp.float32),
                pltpu.VMEM((4 * (WIDTH * 8 + bx * WIDTH + 2 * NEAR * NEAR), nz), jnp.float32),
                pltpu.VMEM((bx + 2 * NEAR, 16, nz), jnp.float32),
                pltpu.VMEM((bx + 2 * NEAR, 16, nz), jnp.float32),
                pltpu.VMEM((bx + 2 * NEAR, 16, nz), jnp.float32),
                pltpu.VMEM((bx, by, nz), jnp.float32),
                pltpu.VMEM((norb, 128, 128), jnp.float32),
                pltpu.VMEM((norb, ny, 1, 128), jnp.float32),
                pltpu.VMEM((norb, nx, 1, 128), jnp.float32),
                pltpu.SemaphoreType.REGULAR((NB // GROUP,)),
                pltpu.SemaphoreType.DMA((2,)),
                pltpu.SemaphoreType.DMA((2,)),
                pltpu.SemaphoreType.DMA((8,)),
                pltpu.SemaphoreType.DMA((2, norb)),
                pltpu.SemaphoreType.DMA((1,)),
                pltpu.SemaphoreType.DMA((norb,)),
                pltpu.SemaphoreType.DMA((1,)),
                pltpu.SemaphoreType.DMA((norb,)),
            ],
            compiler_params=pltpu.CompilerParams(
                collective_id=0, has_side_effects=True, vmem_limit_bytes=48 * 2**20
            ),
        )(*(pltpu.with_memory_space_constraint(a, pltpu.HBM) for a in (orbitals, potential)))

    spec = P(None, "orb", "gx", "gyz", None)
    return jax.shard_map(
        shards, mesh=mesh, in_specs=(spec, P("gx", "gyz", None)), out_specs=(spec, spec), check_vma=False
    )
```

```python
import functools

import jax
import jax.numpy as jnp
from jax import lax
from jax.experimental import pallas as pl
from jax.experimental.pallas import tpu as pltpu
from jax.sharding import PartitionSpec as P

ITERS = 4
NB = 2 * ITERS + 1
SPACING = 0.25
HALF_STEP = 0.05
DIAG = 3.75 / SPACING**2
KAPPA = -0.5 / SPACING**2 * HALF_STEP * (4.0 / 3.0)
FAR = -1.0 / 16.0
MESH = pl.DeviceIdType.MESH
GROUP = 3
WIDTH = 2 * GROUP
NEAR = WIDTH - 2
ROW = 8
RC = 4
IM = 64


_ANGLE = (0.955336489, 0.295520207)
_NODES = (0.0, 0.6761480, -0.6761480, 0.0, 0.1811733, -0.1811733, 0.0, 0.4949747, -0.4949747)
SHIFT = tuple((t * _ANGLE[0], t * _ANGLE[1]) for t in _NODES)


def tri(i, j):
    return j * (j + 1) // 2 + i


def cmul(a, b):
    return (a[0] * b[0] - a[1] * b[1], a[0] * b[1] + a[1] * b[0])


def cconjmul(a, b):
    return (a[0] * b[0] + a[1] * b[1], a[0] * b[1] - a[1] * b[0])


def cdiv(a, b):
    modulus = b[0] * b[0] + b[1] * b[1]
    return ((a[0] * b[0] + a[1] * b[1]) / modulus, (a[1] * b[0] - a[0] * b[1]) / modulus)


def cadd(a, b):
    return (a[0] + b[0], a[1] + b[1])


def csub(a, b):
    return (a[0] - b[0], a[1] - b[1])


def csum(terms):
    while len(terms) > 1:
        terms = [cadd(terms[k], terms[k + 1]) if k + 1 < len(terms) else terms[k] for k in range(0, len(terms), 2)]
    return terms[0]


def shifted_sum(a):
    out = []
    for k in range(len(a)):
        re, im = SHIFT[k + 1]
        t = a[k] if re == 0.0 else cmul((1.0 + re, im), a[k])
        out.append(cadd(t, a[k - 1]) if k else t)
    out.append(a[-1])
    return out


def axpy(a, s, b):
    out = []
    for k in range(max(len(a), len(b))):
        if k >= len(b):
            out.append(a[k])
        else:
            t = cmul(s, b[k])
            out.append(csub(a[k], t) if k < len(a) else (-t[0], -t[1]))
    return out


def recurrences(gram):
    def shadow_dot(a):
        return csum([cmul(gram(0, k), a[k]) for k in range(len(a))])

    one = jnp.ones_like(gram(0, 0)[0])
    zero = jnp.zeros_like(one)
    residual = [(one, zero)]
    direction = residual
    x = []
    rho = gram(0, 0)
    for iteration in range(ITERS):
        image = shifted_sum(direction)
        alpha = cdiv(rho, shadow_dot(image))
        half = axpy(residual, alpha, image)
        second = shifted_sum(half)
        n = len(second)
        g_second = [csum([cmul(gram(k, l), second[l]) for l in range(n)]) for k in range(n)]
        norm = csum([cconjmul(second[k], g_second[k]) for k in range(n)])[0]
        cross = csum([cconjmul(g_second[k], half[k]) for k in range(len(half))])
        omega = (cross[0] / norm, cross[1] / norm)
        minus = lambda s: (-s[0], -s[1])
        x = axpy(axpy(x, minus(alpha), direction), minus(omega), half)
        residual = axpy(half, omega, second)
        if iteration + 1 < ITERS:
            rho_next = shadow_dot(residual)
            beta = cmul(cdiv(rho_next, rho), cdiv(alpha, omega))
            direction = axpy(residual, minus(beta), axpy(direction, omega, image))
            rho = rho_next
    return residual, x


def kernel(
    nx, ny, orb_hbm, pot_hbm, out_ref, *scratch,
):
    (ux, *us) = scratch[:NB + 2 - NB // GROUP]
    us = [ux.at[k // GROUP] if k % GROUP == 0 and k < NB else us.pop(0) for k in range(NB + 1)]
    (stage, pot, ballast, pr, pi, qf, weight, gram, part_y, part_x,
     ready, load_sem, pot_sem, send_sem, recv_sem, ysend_sem, yrecv_sem, xsend_sem, xrecv_sem) = scratch[NB + 2 - NB // GROUP:]
    norb, bx = orb_hbm.shape[1], orb_hbm.shape[2]
    io, ix, iy = lax.axis_index("orb"), lax.axis_index("gx"), lax.axis_index("gyz")
    rows = pl.ds(ROW, 8)

    load_pot = pltpu.make_async_copy(pot_hbm, pot.at[pl.ds(NEAR, bx), rows], load_sem.at[0])
    load_pot.start()
    load_orb = pltpu.make_async_copy(orb_hbm, stage, load_sem.at[1])
    load_orb.start()

    low_x, high_x, low_y, high_y = ix > 0, ix < nx - 1, iy > 0, iy < ny - 1
    exists = {-1: (low_x, low_y), 0: (None, None), 1: (high_x, high_y)}

    def present(dx, dy):
        a, b = exists[dx][0], exists[dy][1]
        return b if a is None else a if b is None else jnp.logical_and(a, b)

    sides = ((1, 1), (1, -1), (-1, 1), (-1, -1), (1, 0), (-1, 0), (0, 1), (0, -1))

    def span(d, length, first, width):
        if d == 0:
            return pl.ds(first, length), pl.ds(first, length)
        if d > 0:
            return pl.ds(first + length - width, width), pl.ds(first - width, width)
        return pl.ds(first, width), pl.ds(first + length, width)

    def inside(dx, dy):
        ok = None
        for d, at, n in ((dx, ix, nx), (dy, iy, ny)):
            if d:
                here = at < n - d if d > 0 else at >= -d
                ok = here if ok is None else jnp.logical_and(ok, here)
        return ok

    def greet(sem, offsets):
        for dx, dy in offsets:
            @pl.when(inside(dx, dy))
            def _():
                pl.semaphore_signal(sem, inc=1, device_id=(io, ix + dx, iy + dy), device_id_type=MESH)

    def await_greetings(sem, offsets):
        pl.semaphore_wait(sem, sum(inside(dx, dy).astype(jnp.int32) for dx, dy in offsets))

    def around(dx, dy):
        return [(dx, 0), (-dx, 0), (0, dy), (0, -dy)]

    first = list(sides) + [(0, 2), (0, -2)]
    rounds = (around(1, 1) + [(0, 2), (0, -2)], around(2, 4), around(4, 8))
    assert nx <= 8 and ny <= 16
    barrier = pltpu.get_barrier_semaphore()
    greet(barrier, first)

    def pot_halo(side):
        dx, dy = sides[side]
        width = NEAR - 2 if dx and dy else NEAR
        (sx, tx), (sr, tr) = span(dx, bx, NEAR, width), span(dy, 8, ROW, width)
        return pltpu.make_async_remote_copy(
            src_ref=pot.at[sx, sr], dst_ref=pot.at[tx, tr],
            send_sem=pot_sem.at[0], recv_sem=pot_sem.at[1],
            device_id=(io, ix + dx, iy + dy), device_id_type=MESH,
        )

    def halo_spans(side):
        dx, dy = sides[side]
        if not (dx and dy):
            return [(span(dx, bx, WIDTH, WIDTH), span(dy, 8, ROW, WIDTH))]
        pieces = []
        for k in range(GROUP - 1):
            from_x = span(dx, bx, WIDTH, 2)
            from_x = tuple(pl.ds(at.start - 2 * k * dx, 2) for at in from_x)
            pieces.append((from_x, span(dy, 8, ROW, NEAR - 2 * k)))
        return pieces

    def halo(g, o, side):
        dx, dy = sides[side]
        ref = us[GROUP * g]
        return [
            pltpu.make_async_remote_copy(
                src_ref=ref.at[o, sx, :, sr], dst_ref=ref.at[o, tx, :, tr],
                send_sem=send_sem.at[side], recv_sem=recv_sem.at[g % 2, o],
                device_id=(io, ix + dx, iy + dy), device_id_type=MESH,
            )
            for (sx, tx), (sr, tr) in halo_spans(side)
        ]

    corner_cells = sum(2 * (NEAR - 2 * k) for k in range(GROUP - 1))

    def each_side(act):
        for side, (dx, dy) in enumerate(sides):
            @pl.when(present(dx, dy))
            def _():
                act(side)

    def send(g, o):
        each_side(lambda side: [copy.start() for copy in halo(g, o, side)])

    both_x, both_y = jnp.logical_and(low_x, high_x), jnp.logical_and(low_y, high_y)

    def await_sides(sem, planes, wide, corner):
        for nsx in (1, 2):
            for nsy in (1, 2):
                here = jnp.logical_and(both_x if nsx == 2 else jnp.logical_not(both_x),
                                       both_y if nsy == 2 else jnp.logical_not(both_y))
                total = planes * (nsx * wide * 8 + nsy * bx * wide + nsx * nsy * corner)
                ref = ballast.at[pl.ds(0, total)]

                @pl.when(here)
                def _():
                    pltpu.make_async_copy(ref, ref, sem).wait()

    def receive(g, o):
        await_sides(recv_sem.at[g % 2, o], 2, WIDTH, corner_cells)

    def clear(x0, nplanes, r0, nrows):
        def body(x, carry):
            for g in range(NB // GROUP):
                for o in range(norb):
                    us[GROUP * g][o, x, :, pl.ds(r0, nrows), :] = jnp.zeros((2, nrows, 128), jnp.float32)
            return carry
        lax.fori_loop(x0, x0 + nplanes, body, 0)

    def clear_pot(x0, nplanes, r0, nrows):
        pot[pl.ds(x0, nplanes), pl.ds(r0, nrows), :] = jnp.zeros((nplanes, nrows, 128), jnp.float32)

    for has, x0 in ((low_x, 0), (high_x, bx + WIDTH)):
        @pl.when(jnp.logical_not(has))
        def _():
            clear(x0, WIDTH, ROW - WIDTH, 8 + 2 * WIDTH)
            clear_pot(0 if x0 == 0 else bx + NEAR, NEAR, ROW - NEAR, 8 + 2 * NEAR)
    for has, r0 in ((low_y, ROW - WIDTH), (high_y, ROW + 8)):
        @pl.when(jnp.logical_not(has))
        def _():
            clear(0, bx + 2 * WIDTH, r0, WIDTH)
            clear_pot(0, bx + 2 * NEAR, ROW - NEAR if r0 < ROW else ROW + 8, NEAR)
    gram[...] = jnp.zeros_like(gram)

    load_pot.wait()
    load_orb.wait()

    def unpack(o):
        for x in range(bx):
            for c in range(2):
                us[0][o, x + WIDTH, c, rows] = stage[c, o, x]

    unpack(0)
    await_greetings(barrier, first)
    each_side(lambda side: pot_halo(side).start())
    send(0, 0)
    for o in range(1, norb):
        unpack(o)
        send(0, o)
    greet(ready.at[0], rounds[0])

    zero, one = jnp.float32(0.0), jnp.float32(1.0)
    row = lax.broadcasted_iota(jnp.int32, (8, 128), 0)
    keep_rows = (
        jnp.where(jnp.logical_or(row >= ROW - RC, low_y), one, zero),
        jnp.where(jnp.logical_or(row < 8 - (ROW - RC), high_y), one, zero),
    )

    def coefficients(x, keep):
        for t in range(2):
            q = HALF_STEP * (DIAG + pot[x, pl.ds(RC + 8 * t, 8)])
            p = KAPPA / (1.0 + q * q) * keep_rows[t] * keep
            tile = pl.ds(8 * t, 8)
            qf[x, tile] = q
            pr[x, tile] = p
            pi[x, tile] = -q * p

    def weights(x, carry):
        q = HALF_STEP * (DIAG + pot[x + NEAR, rows])
        weight[x] = (1.0 + q * q) * (1.0 / KAPPA**2)
        return carry

    lax.fori_loop(0, bx, weights, 0, unroll=4)
    await_greetings(ready.at[0], rounds[0])
    greet(ready.at[1], rounds[1])
    await_sides(pot_sem.at[1], 1, NEAR, (NEAR - 2) ** 2)
    lax.fori_loop(0, NEAR, lambda x, c: (coefficients(x, jnp.where(low_x, one, zero)), c)[1], 0)
    lax.fori_loop(NEAR, bx + NEAR, lambda x, c: (coefficients(x, one), c)[1], 0, unroll=4)
    lax.fori_loop(bx + NEAR, bx + 2 * NEAR, lambda x, c: (coefficients(x, jnp.where(high_x, one, zero)), c)[1], 0)

    lane = lax.broadcasted_iota(jnp.int32, (8, 128), 1)
    near = (jnp.where(lane >= 1, one, zero), jnp.where(lane < 127, one, zero))
    far = (jnp.where(lane >= 2, FAR * one, zero), jnp.where(lane < 126, FAR * one, zero))

    def stencil(u, o, x, c, r):
        def at(dx, dr):
            return u[o, x + WIDTH + dx, c, pl.ds(r + dr, 8)]
        center = at(0, 0)
        s1 = (at(-1, 0) + at(1, 0)) + (at(0, -1) + at(0, 1))
        s2 = (at(-2, 0) + at(2, 0)) + (at(0, -2) + at(0, 2))
        z1 = near[0] * pltpu.roll(center, 1, 1) + near[1] * pltpu.roll(center, 127, 1)
        z2 = far[0] * pltpu.roll(center, 2, 1) + far[1] * pltpu.roll(center, 126, 1)
        return center, (s1 + z1) + (FAR * s2 + z2)

    def advance(s, o):
        u, margin = us[s], WIDTH - 2 - 2 * (s % GROUP)
        for x in range(-margin, bx + margin):
            out = -x if x < 0 else x - bx + 1 if x >= bx else 0
            beyond = margin - 2 * ((out + 1) // 2)
            for r in (ROW,) if beyond == 0 else (RC, RC + 8):
                u_re, t_re = stencil(u, o, x, 0, r)
                u_im, t_im = stencil(u, o, x, 1, r)
                tile = pl.ds(r - RC, 8)
                a, b = pr[x + NEAR, tile], pi[x + NEAR, tile]
                if s == 0:
                    q = qf[x + NEAR, tile]
                    w_re = 2.0 * (KAPPA * t_im + q * u_im)
                    w_im = -2.0 * (KAPPA * t_re + q * u_re)
                    v_re, v_im = a * w_re - b * w_im, a * w_im + b * w_re
                else:
                    re, im = SHIFT[s]
                    v_re, v_im = -(a * t_im + b * t_re), a * t_re - b * t_im
                    if re != 0.0:
                        v_re = (im * u_im - a * t_im) - (re * u_re + b * t_re)
                        v_im = (a * t_re - re * u_im) - (im * u_re + b * t_im)
                us[s + 1][o, x + WIDTH, 0, pl.ds(r, 8)] = v_re
                us[s + 1][o, x + WIDTH, 1, pl.ds(r, 8)] = v_im

    def vector(k, o, x):
        return us[k + 1][o, x + WIDTH, 0, rows], us[k + 1][o, x + WIDTH, 1, rows]

    def products(o, pairs):
        acc = {}
        for x in range(bx):
            v = {k: vector(k, o, x) for k in sorted({k for pair in pairs for k in pair})}
            weighted = {i: (weight[x] * v[i][0], weight[x] * v[i][1]) for i in sorted({i for i, _ in pairs})}
            for i, j in pairs:
                (ar, ai), (br, bi) = weighted[i], v[j]
                terms = [ar * br + ai * bi] + ([ar * bi - ai * br] if i != j else [])
                for part, term in enumerate(terms):
                    key = (i, j, part, x % 2)
                    acc[key] = acc[key] + term if key in acc else term
        for i, j in pairs:
            for part in range(1 if i == j else 2):
                tile = acc[i, j, part, 0] + acc[i, j, part, 1]
                gram[o, pl.ds(part * IM + tri(i, j), 1)] = jnp.sum(tile, axis=0, keepdims=True)

    def column_products(g, o):
        new = range(GROUP * g, GROUP * g + GROUP)
        for i in range(GROUP * g):
            products(o, [(i, j) for j in new])
        products(o, [(i, j) for i in new for j in new if i <= j][:3])
        products(o, [(i, j) for i in new for j in new if i <= j][3:])

    def exchange(part, me, n, target, ssem, rsem):
        def start(o, row):
            part[o, me] = row
            for d in sorted(range(1, n), key=lambda d: -min(d, n - d)):
                pltpu.make_async_remote_copy(
                    src_ref=part.at[o, me], dst_ref=part.at[o, me], send_sem=ssem, recv_sem=rsem.at[o],
                    device_id=target(lax.rem(me + d, n)), device_id_type=MESH,
                ).start()

        def total(o):
            others = part.at[o, pl.ds(0, n - 1)]
            pltpu.make_async_copy(others, others, rsem.at[o]).wait()
            terms = [part[o, k] for k in range(n)]
            while len(terms) > 1:
                terms = [terms[k] + terms[k + 1] for k in range(0, len(terms), 2)]
            return terms[0]

        def drain():
            others = part.at[:, pl.ds(0, n - 1)]
            pltpu.make_async_copy(others, others, ssem).wait()

        return start, total, drain

    start_y, total_y, drain_y = exchange(part_y, iy, ny, lambda t: (io, ix, t), ysend_sem.at[0], yrecv_sem)
    start_x, total_x, drain_x = exchange(part_x, ix, nx, lambda t: (io, t, iy), xsend_sem.at[0], xrecv_sem)

    def start_reduction(o):
        sums = lax.dot_general(
            jnp.ones((8, 128), jnp.float32), gram[o], (((1,), (1,)), ((), ())),
            precision=lax.Precision.HIGHEST, preferred_element_type=jnp.float32,
        )
        start_y(o, sums[0:1])

    groups = NB // GROUP
    for g in range(groups):
        def orbital(o, carry):
            receive(g, o)
            for s in range(GROUP * g, GROUP * g + GROUP):
                advance(s, o)
            if g < groups - 1:
                send(g + 1, o)
            else:
                column_products(g, o)
                start_reduction(o)
            return carry
        lax.fori_loop(0, norb, orbital, 0)
        if g == 0:
            await_greetings(ready.at[1], rounds[1])
            greet(ready.at[2], rounds[2])
        if g == 1:
            await_greetings(ready.at[2], rounds[2])
        if g < groups - 1:
            def gram_columns(o, carry):
                column_products(g, o)
                return carry
            lax.fori_loop(0, norb, gram_columns, 0)

    def second_stage(o, carry):
        start_x(o, total_y(o))
        return carry

    lax.fori_loop(0, norb, second_stage, 0)

    await_sides(pot_sem.at[0], 1, NEAR, (NEAR - 2) ** 2)
    for side, (dx, dy) in enumerate(sides):
        cells = sum(sx.size * sr.size for (sx, _), (sr, _) in halo_spans(side))
        sent = ux.at[:, :, pl.ds(0, cells // 4), :, pl.ds(ROW, 4)]

        @pl.when(present(dx, dy))
        def _():
            pltpu.make_async_copy(sent, sent, send_sem.at[side]).wait()
    drain_y()

    def finish(o, carry):
        total = jnp.broadcast_to(total_x(o), (8, 128))

        def spread(e):
            return jnp.broadcast_to(total[:, e:e + 1], (8, 128))

        entries = {}
        for j in range(NB):
            for i in range(j + 1):
                re = spread(tri(i, j))
                im = jnp.zeros_like(re) if i == j else spread(IM + tri(i, j))
                entries[i, j] = (re, im)
                if i != j:
                    entries[j, i] = (re, -im)
        res_coef, x_coef = recurrences(lambda i, j: entries[i, j])
        rc = [(c[0] * (1.0 / KAPPA), c[1] * (1.0 / KAPPA)) for c in res_coef]
        xc = [(c[0] * (1.0 / KAPPA), c[1] * (1.0 / KAPPA)) for c in x_coef]

        def combine(x, carry):
            vectors = [vector(k, o, x) for k in range(NB)]
            re, im = csum([cmul(rc[k], vectors[k]) for k in range(NB)])
            inc = csum([cmul(xc[k], vectors[k]) for k in range(NB - 1)])
            q = qf[x + NEAR, pl.ds(ROW - RC, 8)]
            out_ref[1, 0, o, x] = re - q * im
            out_ref[1, 1, o, x] = im + q * re
            for c in range(2):
                out_ref[0, c, o, x] = stage[c, o, x] + inc[c]
            return carry

        lax.fori_loop(0, bx, combine, 0, unroll=4)
        return carry

    lax.fori_loop(0, norb, finish, 0)
    drain_x()


def solution(mesh):
    nx, ny = mesh.shape["gx"], mesh.shape["gyz"]

    def shards(orbitals, potential):
        _, norb, bx, by, nz = orbitals.shape
        both = pl.pallas_call(
            functools.partial(kernel, nx, ny),
            out_shape=jax.ShapeDtypeStruct((2, *orbitals.shape), jnp.float32),
            in_specs=[pl.BlockSpec(memory_space=pltpu.HBM)] * 2,
            out_specs=pl.BlockSpec(memory_space=pltpu.VMEM),
            scratch_shapes=[
                pltpu.VMEM((NB // GROUP, norb, bx + 2 * WIDTH, 2, by + 16, nz), jnp.float32)
            ] + [
                pltpu.VMEM((norb, bx + 2 * WIDTH, 2, by + 16, nz), jnp.float32) for _ in range(NB + 1 - NB // GROUP)
            ] + [
                pltpu.VMEM(orbitals.shape, jnp.float32),
                pltpu.VMEM((bx + 2 * NEAR, by + 16, nz), jnp.float32),
                pltpu.VMEM((4 * (WIDTH * 8 + bx * WIDTH + 2 * NEAR * NEAR), nz), jnp.float32),
                pltpu.VMEM((bx + 2 * NEAR, 16, nz), jnp.float32),
                pltpu.VMEM((bx + 2 * NEAR, 16, nz), jnp.float32),
                pltpu.VMEM((bx + 2 * NEAR, 16, nz), jnp.float32),
                pltpu.VMEM((bx, by, nz), jnp.float32),
                pltpu.VMEM((norb, 128, 128), jnp.float32),
                pltpu.VMEM((norb, ny, 1, 128), jnp.float32),
                pltpu.VMEM((norb, nx, 1, 128), jnp.float32),
                pltpu.SemaphoreType.REGULAR((NB // GROUP,)),
                pltpu.SemaphoreType.DMA((2,)),
                pltpu.SemaphoreType.DMA((2,)),
                pltpu.SemaphoreType.DMA((8,)),
                pltpu.SemaphoreType.DMA((2, norb)),
                pltpu.SemaphoreType.DMA((1,)),
                pltpu.SemaphoreType.DMA((norb,)),
                pltpu.SemaphoreType.DMA((1,)),
                pltpu.SemaphoreType.DMA((norb,)),
            ],
            compiler_params=pltpu.CompilerParams(
                collective_id=0, has_side_effects=True, vmem_limit_bytes=48 * 2**20
            ),
        )(*(pltpu.with_memory_space_constraint(a, pltpu.HBM) for a in (orbitals, potential)))
        return both[0], both[1]

    spec = P(None, "orb", "gx", "gyz", None)
    return jax.shard_map(
        shards, mesh=mesh, in_specs=(spec, P("gx", "gyz", None)), out_specs=(spec, spec), check_vma=False
    )
```

```python
import functools

import jax
import jax.numpy as jnp
from jax import lax
from jax.experimental import pallas as pl
from jax.experimental.pallas import tpu as pltpu
from jax.sharding import PartitionSpec as P

ITERS = 4
NB = 2 * ITERS + 1
SPACING = 0.25
HALF_STEP = 0.05
DIAG = 3.75 / SPACING**2
KAPPA = -0.5 / SPACING**2 * HALF_STEP * (4.0 / 3.0)
FAR = -1.0 / 16.0
MESH = pl.DeviceIdType.MESH
GROUP = 3
WIDTH = 2 * GROUP
NEAR = WIDTH - 2
ROW = 8
RC = 4
IM = 64


_ANGLE = (0.955336489, 0.295520207)
_NODES = (0.0, 0.6761480, -0.6761480, 0.0, 0.1811733, -0.1811733, 0.0, 0.4949747, -0.4949747)
SHIFT = tuple((t * _ANGLE[0], t * _ANGLE[1]) for t in _NODES)


def tri(i, j):
    return j * (j + 1) // 2 + i


def cmul(a, b):
    return (a[0] * b[0] - a[1] * b[1], a[0] * b[1] + a[1] * b[0])


def cconjmul(a, b):
    return (a[0] * b[0] + a[1] * b[1], a[0] * b[1] - a[1] * b[0])


def cdiv(a, b):
    modulus = b[0] * b[0] + b[1] * b[1]
    return ((a[0] * b[0] + a[1] * b[1]) / modulus, (a[1] * b[0] - a[0] * b[1]) / modulus)


def cadd(a, b):
    return (a[0] + b[0], a[1] + b[1])


def csub(a, b):
    return (a[0] - b[0], a[1] - b[1])


def csum(terms):
    while len(terms) > 1:
        terms = [cadd(terms[k], terms[k + 1]) if k + 1 < len(terms) else terms[k] for k in range(0, len(terms), 2)]
    return terms[0]


def shifted_sum(a):
    out = []
    for k in range(len(a)):
        re, im = SHIFT[k + 1]
        t = a[k] if re == 0.0 else cmul((1.0 + re, im), a[k])
        out.append(cadd(t, a[k - 1]) if k else t)
    out.append(a[-1])
    return out


def axpy(a, s, b):
    out = []
    for k in range(max(len(a), len(b))):
        if k >= len(b):
            out.append(a[k])
        else:
            t = cmul(s, b[k])
            out.append(csub(a[k], t) if k < len(a) else (-t[0], -t[1]))
    return out


def recurrences(gram):
    def shadow_dot(a):
        return csum([cmul(gram(0, k), a[k]) for k in range(len(a))])

    one = jnp.ones_like(gram(0, 0)[0])
    zero = jnp.zeros_like(one)
    residual = [(one, zero)]
    direction = residual
    x = []
    rho = gram(0, 0)
    for iteration in range(ITERS):
        image = shifted_sum(direction)
        alpha = cdiv(rho, shadow_dot(image))
        half = axpy(residual, alpha, image)
        second = shifted_sum(half)
        n = len(second)
        g_second = [csum([cmul(gram(k, l), second[l]) for l in range(n)]) for k in range(n)]
        norm = csum([cconjmul(second[k], g_second[k]) for k in range(n)])[0]
        cross = csum([cconjmul(g_second[k], half[k]) for k in range(len(half))])
        omega = (cross[0] / norm, cross[1] / norm)
        minus = lambda s: (-s[0], -s[1])
        x = axpy(axpy(x, minus(alpha), direction), minus(omega), half)
        residual = axpy(half, omega, second)
        if iteration + 1 < ITERS:
            rho_next = shadow_dot(residual)
            beta = cmul(cdiv(rho_next, rho), cdiv(alpha, omega))
            direction = axpy(residual, minus(beta), axpy(direction, omega, image))
            rho = rho_next
    return residual, x


def kernel(
    nx, ny, orb_hbm, pot_hbm, out_ref, *scratch,
):
    (ux, *us) = scratch[:NB + 2 - NB // GROUP]
    us = [ux.at[k // GROUP] if k % GROUP == 0 and k < NB else us.pop(0) for k in range(NB + 1)]
    (stage, pot, ballast, pr, pi, qf, weight, gram, part_y, part_x,
     ready, load_sem, pot_sem, send_sem, recv_sem, ysend_sem, yrecv_sem, xsend_sem, xrecv_sem) = scratch[NB + 2 - NB // GROUP:]
    norb, bx = orb_hbm.shape[1], orb_hbm.shape[2]
    io, ix, iy = lax.axis_index("orb"), lax.axis_index("gx"), lax.axis_index("gyz")
    rows = pl.ds(ROW, 8)

    load_pot = pltpu.make_async_copy(pot_hbm, pot.at[pl.ds(NEAR, bx), rows], load_sem.at[0])
    load_pot.start()
    load_orb = pltpu.make_async_copy(orb_hbm, stage, load_sem.at[1])
    load_orb.start()

    low_x, high_x, low_y, high_y = ix > 0, ix < nx - 1, iy > 0, iy < ny - 1
    exists = {-1: (low_x, low_y), 0: (None, None), 1: (high_x, high_y)}

    def present(dx, dy):
        a, b = exists[dx][0], exists[dy][1]
        return b if a is None else a if b is None else jnp.logical_and(a, b)

    sides = ((1, 1), (1, -1), (-1, 1), (-1, -1), (1, 0), (-1, 0), (0, 1), (0, -1))

    def span(d, length, first, width):
        if d == 0:
            return pl.ds(first, length), pl.ds(first, length)
        if d > 0:
            return pl.ds(first + length - width, width), pl.ds(first - width, width)
        return pl.ds(first, width), pl.ds(first + length, width)

    def inside(dx, dy):
        ok = None
        for d, at, n in ((dx, ix, nx), (dy, iy, ny)):
            if d:
                here = at < n - d if d > 0 else at >= -d
                ok = here if ok is None else jnp.logical_and(ok, here)
        return ok

    def greet(sem, offsets):
        for dx, dy in offsets:
            @pl.when(inside(dx, dy))
            def _():
                pl.semaphore_signal(sem, inc=1, device_id=(io, ix + dx, iy + dy), device_id_type=MESH)

    def await_greetings(sem, offsets):
        pl.semaphore_wait(sem, sum(inside(dx, dy).astype(jnp.int32) for dx, dy in offsets))

    def around(dx, dy):
        return [(dx, 0), (-dx, 0), (0, dy), (0, -dy)]

    first = list(sides) + [(0, 2), (0, -2)]
    rounds = (around(1, 1) + [(0, 2), (0, -2)], around(2, 4), around(4, 8))
    assert nx <= 8 and ny <= 16
    barrier = pltpu.get_barrier_semaphore()
    greet(barrier, first)

    def pot_halo(side):
        dx, dy = sides[side]
        width = NEAR - 2 if dx and dy else NEAR
        (sx, tx), (sr, tr) = span(dx, bx, NEAR, width), span(dy, 8, ROW, width)
        return pltpu.make_async_remote_copy(
            src_ref=pot_hbm.at[pl.ds(sx.start - NEAR, sx.size), pl.ds(sr.start - ROW, sr.size)],
            dst_ref=pot.at[tx, tr],
            send_sem=pot_sem.at[0], recv_sem=pot_sem.at[1],
            device_id=(io, ix + dx, iy + dy), device_id_type=MESH,
        )

    def halo_spans(side):
        dx, dy = sides[side]
        if not (dx and dy):
            return [(span(dx, bx, WIDTH, WIDTH), span(dy, 8, ROW, WIDTH))]
        pieces = []
        for k in range(GROUP - 1):
            from_x = span(dx, bx, WIDTH, 2)
            from_x = tuple(pl.ds(at.start - 2 * k * dx, 2) for at in from_x)
            pieces.append((from_x, span(dy, 8, ROW, NEAR - 2 * k)))
        return pieces

    def halo(g, o, side):
        dx, dy = sides[side]
        ref = us[GROUP * g]
        return [
            pltpu.make_async_remote_copy(
                src_ref=ref.at[o, sx, :, sr], dst_ref=ref.at[o, tx, :, tr],
                send_sem=send_sem.at[side], recv_sem=recv_sem.at[g % 2, o],
                device_id=(io, ix + dx, iy + dy), device_id_type=MESH,
            )
            for (sx, tx), (sr, tr) in halo_spans(side)
        ]

    corner_cells = sum(2 * (NEAR - 2 * k) for k in range(GROUP - 1))

    def each_side(act):
        for side, (dx, dy) in enumerate(sides):
            @pl.when(present(dx, dy))
            def _():
                act(side)

    def send(g, o):
        each_side(lambda side: [copy.start() for copy in halo(g, o, side)])

    both_x, both_y = jnp.logical_and(low_x, high_x), jnp.logical_and(low_y, high_y)

    def await_sides(sem, planes, wide, corner):
        for nsx in (1, 2):
            for nsy in (1, 2):
                here = jnp.logical_and(both_x if nsx == 2 else jnp.logical_not(both_x),
                                       both_y if nsy == 2 else jnp.logical_not(both_y))
                total = planes * (nsx * wide * 8 + nsy * bx * wide + nsx * nsy * corner)
                ref = ballast.at[pl.ds(0, total)]

                @pl.when(here)
                def _():
                    pltpu.make_async_copy(ref, ref, sem).wait()

    def receive(g, o):
        await_sides(recv_sem.at[g % 2, o], 2, WIDTH, corner_cells)

    await_greetings(barrier, first)
    each_side(lambda side: pot_halo(side).start())

    def clear(x0, nplanes, r0, nrows):
        def body(x, carry):
            for g in range(NB // GROUP):
                for o in range(norb):
                    us[GROUP * g][o, x, :, pl.ds(r0, nrows), :] = jnp.zeros((2, nrows, 128), jnp.float32)
            return carry
        lax.fori_loop(x0, x0 + nplanes, body, 0)

    def clear_pot(x0, nplanes, r0, nrows):
        pot[pl.ds(x0, nplanes), pl.ds(r0, nrows), :] = jnp.zeros((nplanes, nrows, 128), jnp.float32)

    for has, x0 in ((low_x, 0), (high_x, bx + WIDTH)):
        @pl.when(jnp.logical_not(has))
        def _():
            clear(x0, WIDTH, ROW - WIDTH, 8 + 2 * WIDTH)
            clear_pot(0 if x0 == 0 else bx + NEAR, NEAR, ROW - NEAR, 8 + 2 * NEAR)
    for has, r0 in ((low_y, ROW - WIDTH), (high_y, ROW + 8)):
        @pl.when(jnp.logical_not(has))
        def _():
            clear(0, bx + 2 * WIDTH, r0, WIDTH)
            clear_pot(0, bx + 2 * NEAR, ROW - NEAR if r0 < ROW else ROW + 8, NEAR)

    load_pot.wait()
    load_orb.wait()

    def unpack(o):
        for x in range(bx):
            for c in range(2):
                us[0][o, x + WIDTH, c, rows] = stage[c, o, x]

    unpack(0)
    send(0, 0)
    for o in range(1, norb):
        unpack(o)
        send(0, o)
    greet(ready.at[0], rounds[0])

    zero, one = jnp.float32(0.0), jnp.float32(1.0)
    row = lax.broadcasted_iota(jnp.int32, (8, 128), 0)
    keep_rows = (
        jnp.where(jnp.logical_or(row >= ROW - RC, low_y), one, zero),
        jnp.where(jnp.logical_or(row < 8 - (ROW - RC), high_y), one, zero),
    )

    def coefficients(x, keep):
        for t in range(2):
            q = HALF_STEP * (DIAG + pot[x, pl.ds(RC + 8 * t, 8)])
            p = KAPPA / (1.0 + q * q) * keep_rows[t] * keep
            tile = pl.ds(8 * t, 8)
            qf[x, tile] = q
            pr[x, tile] = p
            pi[x, tile] = -q * p

    def weights(x, carry):
        q = HALF_STEP * (DIAG + pot[x + NEAR, rows])
        weight[x] = (1.0 + q * q) * (1.0 / KAPPA**2)
        return carry

    lax.fori_loop(0, bx, weights, 0, unroll=4)
    await_greetings(ready.at[0], rounds[0])
    greet(ready.at[1], rounds[1])
    await_sides(pot_sem.at[1], 1, NEAR, (NEAR - 2) ** 2)
    lax.fori_loop(0, NEAR, lambda x, c: (coefficients(x, jnp.where(low_x, one, zero)), c)[1], 0)
    lax.fori_loop(NEAR, bx + NEAR, lambda x, c: (coefficients(x, one), c)[1], 0, unroll=4)
    lax.fori_loop(bx + NEAR, bx + 2 * NEAR, lambda x, c: (coefficients(x, jnp.where(high_x, one, zero)), c)[1], 0)

    lane = lax.broadcasted_iota(jnp.int32, (8, 128), 1)
    near = (jnp.where(lane >= 1, one, zero), jnp.where(lane < 127, one, zero))
    far = (jnp.where(lane >= 2, FAR * one, zero), jnp.where(lane < 126, FAR * one, zero))

    def stencil(u, o, x, c, r):
        def at(dx, dr):
            return u[o, x + WIDTH + dx, c, pl.ds(r + dr, 8)]
        center = at(0, 0)
        s1 = (at(-1, 0) + at(1, 0)) + (at(0, -1) + at(0, 1))
        s2 = (at(-2, 0) + at(2, 0)) + (at(0, -2) + at(0, 2))
        z1 = near[0] * pltpu.roll(center, 1, 1) + near[1] * pltpu.roll(center, 127, 1)
        z2 = far[0] * pltpu.roll(center, 2, 1) + far[1] * pltpu.roll(center, 126, 1)
        return center, (s1 + z1) + (FAR * s2 + z2)

    def advance(s, o):
        u, margin = us[s], WIDTH - 2 - 2 * (s % GROUP)
        for x in range(-margin, bx + margin):
            out = -x if x < 0 else x - bx + 1 if x >= bx else 0
            beyond = margin - 2 * ((out + 1) // 2)
            for r in (ROW,) if beyond == 0 else (RC, RC + 8):
                u_re, t_re = stencil(u, o, x, 0, r)
                u_im, t_im = stencil(u, o, x, 1, r)
                tile = pl.ds(r - RC, 8)
                a, b = pr[x + NEAR, tile], pi[x + NEAR, tile]
                if s == 0:
                    q = qf[x + NEAR, tile]
                    w_re = 2.0 * (KAPPA * t_im + q * u_im)
                    w_im = -2.0 * (KAPPA * t_re + q * u_re)
                    v_re, v_im = a * w_re - b * w_im, a * w_im + b * w_re
                else:
                    re, im = SHIFT[s]
                    v_re, v_im = -(a * t_im + b * t_re), a * t_re - b * t_im
                    if re != 0.0:
                        v_re = (im * u_im - a * t_im) - (re * u_re + b * t_re)
                        v_im = (a * t_re - re * u_im) - (im * u_re + b * t_im)
                us[s + 1][o, x + WIDTH, 0, pl.ds(r, 8)] = v_re
                us[s + 1][o, x + WIDTH, 1, pl.ds(r, 8)] = v_im

    def vector(k, o, x):
        return us[k + 1][o, x + WIDTH, 0, rows], us[k + 1][o, x + WIDTH, 1, rows]

    def products(o, pairs):
        acc = {}
        for x in range(bx):
            v = {k: vector(k, o, x) for k in sorted({k for pair in pairs for k in pair})}
            weighted = {i: (weight[x] * v[i][0], weight[x] * v[i][1]) for i in sorted({i for i, _ in pairs})}
            for i, j in pairs:
                (ar, ai), (br, bi) = weighted[i], v[j]
                terms = [ar * br + ai * bi] + ([ar * bi - ai * br] if i != j else [])
                for part, term in enumerate(terms):
                    key = (i, j, part, x % 2)
                    acc[key] = acc[key] + term if key in acc else term
        for i, j in pairs:
            for part in range(1 if i == j else 2):
                tile = acc[i, j, part, 0] + acc[i, j, part, 1]
                gram[o, pl.ds(part * IM + tri(i, j), 1)] = jnp.sum(tile, axis=0, keepdims=True)

    def column_products(g, o):
        new = range(GROUP * g, GROUP * g + GROUP)
        for i in range(GROUP * g):
            products(o, [(i, j) for j in new])
        products(o, [(i, j) for i in new for j in new if i <= j][:3])
        products(o, [(i, j) for i in new for j in new if i <= j][3:])

    def exchange(part, me, n, target, ssem, rsem):
        def start(o, row):
            part[o, me] = row
            for d in sorted(range(1, n), key=lambda d: -min(d, n - d)):
                pltpu.make_async_remote_copy(
                    src_ref=part.at[o, me], dst_ref=part.at[o, me], send_sem=ssem, recv_sem=rsem.at[o],
                    device_id=target(lax.rem(me + d, n)), device_id_type=MESH,
                ).start()

        def total(o):
            others = part.at[o, pl.ds(0, n - 1)]
            pltpu.make_async_copy(others, others, rsem.at[o]).wait()
            terms = [part[o, k] for k in range(n)]
            while len(terms) > 1:
                terms = [terms[k] + terms[k + 1] for k in range(0, len(terms), 2)]
            return terms[0]

        def drain():
            others = part.at[:, pl.ds(0, n - 1)]
            pltpu.make_async_copy(others, others, ssem).wait()

        return start, total, drain

    start_y, total_y, drain_y = exchange(part_y, iy, ny, lambda t: (io, ix, t), ysend_sem.at[0], yrecv_sem)
    start_x, total_x, drain_x = exchange(part_x, ix, nx, lambda t: (io, t, iy), xsend_sem.at[0], xrecv_sem)

    def start_reduction(o):
        sums = lax.dot_general(
            jnp.ones((8, 128), jnp.float32), gram[o], (((1,), (1,)), ((), ())),
            precision=lax.Precision.HIGHEST, preferred_element_type=jnp.float32,
        )
        start_y(o, sums[0:1])

    groups = NB // GROUP
    for g in range(groups):
        def orbital(o, carry):
            receive(g, o)
            for s in range(GROUP * g, GROUP * g + GROUP):
                advance(s, o)
            if g < groups - 1:
                send(g + 1, o)
            else:
                column_products(g, o)
                start_reduction(o)
            return carry
        lax.fori_loop(0, norb, orbital, 0)
        if g == 0:
            await_greetings(ready.at[1], rounds[1])
            greet(ready.at[2], rounds[2])
        if g == 1:
            await_greetings(ready.at[2], rounds[2])
        if g < groups - 1:
            def gram_columns(o, carry):
                column_products(g, o)
                return carry
            lax.fori_loop(0, norb, gram_columns, 0)

    def second_stage(o, carry):
        start_x(o, total_y(o))
        return carry

    lax.fori_loop(0, norb, second_stage, 0)

    await_sides(pot_sem.at[0], 1, NEAR, (NEAR - 2) ** 2)
    for side, (dx, dy) in enumerate(sides):
        cells = sum(sx.size * sr.size for (sx, _), (sr, _) in halo_spans(side))
        sent = ux.at[:, :, pl.ds(0, cells // 4), :, pl.ds(ROW, 4)]

        @pl.when(present(dx, dy))
        def _():
            pltpu.make_async_copy(sent, sent, send_sem.at[side]).wait()
    drain_y()

    def finish(o, carry):
        total = jnp.broadcast_to(total_x(o), (8, 128))

        def spread(e):
            return jnp.broadcast_to(total[:, e:e + 1], (8, 128))

        entries = {}
        for j in range(NB):
            for i in range(j + 1):
                re = spread(tri(i, j))
                im = jnp.zeros_like(re) if i == j else spread(IM + tri(i, j))
                entries[i, j] = (re, im)
                if i != j:
                    entries[j, i] = (re, -im)
        res_coef, x_coef = recurrences(lambda i, j: entries[i, j])
        rc = [(c[0] * (1.0 / KAPPA), c[1] * (1.0 / KAPPA)) for c in res_coef]
        xc = [(c[0] * (1.0 / KAPPA), c[1] * (1.0 / KAPPA)) for c in x_coef]

        def combine(x, carry):
            vectors = [vector(k, o, x) for k in range(NB)]
            re, im = csum([cmul(rc[k], vectors[k]) for k in range(NB)])
            inc = csum([cmul(xc[k], vectors[k]) for k in range(NB - 1)])
            q = qf[x + NEAR, pl.ds(ROW - RC, 8)]
            out_ref[1, 0, o, x] = re - q * im
            out_ref[1, 1, o, x] = im + q * re
            for c in range(2):
                out_ref[0, c, o, x] = stage[c, o, x] + inc[c]
            return carry

        lax.fori_loop(0, bx, combine, 0, unroll=4)
        return carry

    lax.fori_loop(0, norb, finish, 0)
    drain_x()


def solution(mesh):
    nx, ny = mesh.shape["gx"], mesh.shape["gyz"]

    def shards(orbitals, potential):
        _, norb, bx, by, nz = orbitals.shape
        both = pl.pallas_call(
            functools.partial(kernel, nx, ny),
            out_shape=jax.ShapeDtypeStruct((2, *orbitals.shape), jnp.float32),
            in_specs=[pl.BlockSpec(memory_space=pltpu.HBM)] * 2,
            out_specs=pl.BlockSpec(memory_space=pltpu.VMEM),
            scratch_shapes=[
                pltpu.VMEM((NB // GROUP, norb, bx + 2 * WIDTH, 2, by + 16, nz), jnp.float32)
            ] + [
                pltpu.VMEM((norb, bx + 2 * WIDTH, 2, by + 16, nz), jnp.float32) for _ in range(NB + 1 - NB // GROUP)
            ] + [
                pltpu.VMEM(orbitals.shape, jnp.float32),
                pltpu.VMEM((bx + 2 * NEAR, by + 16, nz), jnp.float32),
                pltpu.VMEM((4 * (WIDTH * 8 + bx * WIDTH + 2 * NEAR * NEAR), nz), jnp.float32),
                pltpu.VMEM((bx + 2 * NEAR, 16, nz), jnp.float32),
                pltpu.VMEM((bx + 2 * NEAR, 16, nz), jnp.float32),
                pltpu.VMEM((bx + 2 * NEAR, 16, nz), jnp.float32),
                pltpu.VMEM((bx, by, nz), jnp.float32),
                pltpu.VMEM((norb, 128, 128), jnp.float32),
                pltpu.VMEM((norb, ny, 1, 128), jnp.float32),
                pltpu.VMEM((norb, nx, 1, 128), jnp.float32),
                pltpu.SemaphoreType.REGULAR((NB // GROUP,)),
                pltpu.SemaphoreType.DMA((2,)),
                pltpu.SemaphoreType.DMA((2,)),
                pltpu.SemaphoreType.DMA((8,)),
                pltpu.SemaphoreType.DMA((2, norb)),
                pltpu.SemaphoreType.DMA((1,)),
                pltpu.SemaphoreType.DMA((norb,)),
                pltpu.SemaphoreType.DMA((1,)),
                pltpu.SemaphoreType.DMA((norb,)),
            ],
            compiler_params=pltpu.CompilerParams(
                collective_id=0, has_side_effects=True, vmem_limit_bytes=48 * 2**20
            ),
        )(*(pltpu.with_memory_space_constraint(a, pltpu.HBM) for a in (orbitals, potential)))
        return both[0], both[1]

    spec = P(None, "orb", "gx", "gyz", None)
    return jax.shard_map(
        shards, mesh=mesh, in_specs=(spec, P("gx", "gyz", None)), out_specs=(spec, spec), check_vma=False
    )
```

```python
import functools

import jax
import jax.numpy as jnp
from jax import lax
from jax.experimental import pallas as pl
from jax.experimental.pallas import tpu as pltpu
from jax.sharding import PartitionSpec as P

ITERS = 4
NB = 2 * ITERS + 1
SPACING = 0.25
HALF_STEP = 0.05
DIAG = 3.75 / SPACING**2
KAPPA = -0.5 / SPACING**2 * HALF_STEP * (4.0 / 3.0)
FAR = -1.0 / 16.0
MESH = pl.DeviceIdType.MESH
GROUP = 3
WIDTH = 2 * GROUP
NEAR = WIDTH - 2
ROW = 8
RC = 4
IM = 64


_ANGLE = (0.955336489, 0.295520207)
_NODES = (0.0, 0.6761480, -0.6761480, 0.0, 0.1811733, -0.1811733, 0.0, 0.4949747, -0.4949747)
SHIFT = tuple((t * _ANGLE[0], t * _ANGLE[1]) for t in _NODES)


def tri(i, j):
    return j * (j + 1) // 2 + i


def cmul(a, b):
    return (a[0] * b[0] - a[1] * b[1], a[0] * b[1] + a[1] * b[0])


def cconjmul(a, b):
    return (a[0] * b[0] + a[1] * b[1], a[0] * b[1] - a[1] * b[0])


def cdiv(a, b):
    modulus = b[0] * b[0] + b[1] * b[1]
    return ((a[0] * b[0] + a[1] * b[1]) / modulus, (a[1] * b[0] - a[0] * b[1]) / modulus)


def cadd(a, b):
    return (a[0] + b[0], a[1] + b[1])


def csub(a, b):
    return (a[0] - b[0], a[1] - b[1])


def csum(terms):
    while len(terms) > 1:
        terms = [cadd(terms[k], terms[k + 1]) if k + 1 < len(terms) else terms[k] for k in range(0, len(terms), 2)]
    return terms[0]


def shifted_sum(a):
    out = []
    for k in range(len(a)):
        re, im = SHIFT[k + 1]
        t = a[k] if re == 0.0 else cmul((1.0 + re, im), a[k])
        out.append(cadd(t, a[k - 1]) if k else t)
    out.append(a[-1])
    return out


def axpy(a, s, b):
    out = []
    for k in range(max(len(a), len(b))):
        if k >= len(b):
            out.append(a[k])
        else:
            t = cmul(s, b[k])
            out.append(csub(a[k], t) if k < len(a) else (-t[0], -t[1]))
    return out


def recurrences(gram):
    def shadow_dot(a):
        return csum([cmul(gram(0, k), a[k]) for k in range(len(a))])

    one = jnp.ones_like(gram(0, 0)[0])
    zero = jnp.zeros_like(one)
    residual = [(one, zero)]
    direction = residual
    x = []
    rho = gram(0, 0)
    for iteration in range(ITERS):
        image = shifted_sum(direction)
        alpha = cdiv(rho, shadow_dot(image))
        half = axpy(residual, alpha, image)
        second = shifted_sum(half)
        n = len(second)
        g_second = [csum([cmul(gram(k, l), second[l]) for l in range(n)]) for k in range(n)]
        norm = csum([cconjmul(second[k], g_second[k]) for k in range(n)])[0]
        cross = csum([cconjmul(g_second[k], half[k]) for k in range(len(half))])
        omega = (cross[0] / norm, cross[1] / norm)
        minus = lambda s: (-s[0], -s[1])
        x = axpy(axpy(x, minus(alpha), direction), minus(omega), half)
        residual = axpy(half, omega, second)
        if iteration + 1 < ITERS:
            rho_next = shadow_dot(residual)
            beta = cmul(cdiv(rho_next, rho), cdiv(alpha, omega))
            direction = axpy(residual, minus(beta), axpy(direction, omega, image))
            rho = rho_next
    return residual, x


def kernel(
    nx, ny, orb_hbm, pot_hbm, out_ref, *scratch,
):
    (ux, *us) = scratch[:NB + 2 - NB // GROUP]
    us = [ux.at[k // GROUP] if k % GROUP == 0 and k < NB else us.pop(0) for k in range(NB + 1)]
    (pot, ballast, pr, pi, qf, weight, gram, part_y, part_x,
     ready, load_sem, pot_sem, send_sem, recv_sem, ysend_sem, yrecv_sem, xsend_sem, xrecv_sem) = scratch[NB + 2 - NB // GROUP:]
    norb, bx = orb_hbm.shape[1], orb_hbm.shape[2]
    io, ix, iy = lax.axis_index("orb"), lax.axis_index("gx"), lax.axis_index("gyz")
    rows = pl.ds(ROW, 8)

    load_pot = pltpu.make_async_copy(pot_hbm, pot.at[pl.ds(NEAR, bx), rows], load_sem.at[0])
    load_pot.start()
    for o in range(norb):
        for c in range(2):
            pltpu.make_async_copy(
                orb_hbm.at[c, o], us[0].at[o, pl.ds(WIDTH, bx), c, rows], load_sem.at[1 + o]
            ).start()

    low_x, high_x, low_y, high_y = ix > 0, ix < nx - 1, iy > 0, iy < ny - 1
    exists = {-1: (low_x, low_y), 0: (None, None), 1: (high_x, high_y)}

    def present(dx, dy):
        a, b = exists[dx][0], exists[dy][1]
        return b if a is None else a if b is None else jnp.logical_and(a, b)

    sides = ((1, 1), (1, -1), (-1, 1), (-1, -1), (1, 0), (-1, 0), (0, 1), (0, -1))

    def span(d, length, first, width):
        if d == 0:
            return pl.ds(first, length), pl.ds(first, length)
        if d > 0:
            return pl.ds(first + length - width, width), pl.ds(first - width, width)
        return pl.ds(first, width), pl.ds(first + length, width)

    def inside(dx, dy):
        ok = None
        for d, at, n in ((dx, ix, nx), (dy, iy, ny)):
            if d:
                here = at < n - d if d > 0 else at >= -d
                ok = here if ok is None else jnp.logical_and(ok, here)
        return ok

    def greet(sem, offsets):
        for dx, dy in offsets:
            @pl.when(inside(dx, dy))
            def _():
                pl.semaphore_signal(sem, inc=1, device_id=(io, ix + dx, iy + dy), device_id_type=MESH)

    def await_greetings(sem, offsets):
        pl.semaphore_wait(sem, sum(inside(dx, dy).astype(jnp.int32) for dx, dy in offsets))

    def around(dx, dy):
        return [(dx, 0), (-dx, 0), (0, dy), (0, -dy)]

    first = list(sides) + [(0, 2), (0, -2)]
    rounds = (around(1, 1) + [(0, 2), (0, -2)], around(2, 4), around(4, 8))
    assert nx <= 8 and ny <= 16
    barrier = pltpu.get_barrier_semaphore()
    greet(barrier, first)

    def pot_halo(side):
        dx, dy = sides[side]
        width = NEAR - 2 if dx and dy else NEAR
        (sx, tx), (sr, tr) = span(dx, bx, NEAR, width), span(dy, 8, ROW, width)
        return pltpu.make_async_remote_copy(
            src_ref=pot.at[sx, sr], dst_ref=pot.at[tx, tr],
            send_sem=pot_sem.at[0], recv_sem=pot_sem.at[1],
            device_id=(io, ix + dx, iy + dy), device_id_type=MESH,
        )

    def halo_spans(side):
        dx, dy = sides[side]
        if not (dx and dy):
            return [(span(dx, bx, WIDTH, WIDTH), span(dy, 8, ROW, WIDTH))]
        pieces = []
        for k in range(GROUP - 1):
            from_x = span(dx, bx, WIDTH, 2)
            from_x = tuple(pl.ds(at.start - 2 * k * dx, 2) for at in from_x)
            pieces.append((from_x, span(dy, 8, ROW, NEAR - 2 * k)))
        return pieces

    def halo(g, o, side):
        dx, dy = sides[side]
        ref = us[GROUP * g]
        return [
            pltpu.make_async_remote_copy(
                src_ref=ref.at[o, sx, :, sr], dst_ref=ref.at[o, tx, :, tr],
                send_sem=send_sem.at[side], recv_sem=recv_sem.at[g % 2, o],
                device_id=(io, ix + dx, iy + dy), device_id_type=MESH,
            )
            for (sx, tx), (sr, tr) in halo_spans(side)
        ]

    corner_cells = sum(2 * (NEAR - 2 * k) for k in range(GROUP - 1))

    def each_side(act):
        for side, (dx, dy) in enumerate(sides):
            @pl.when(present(dx, dy))
            def _():
                act(side)

    def send(g, o):
        each_side(lambda side: [copy.start() for copy in halo(g, o, side)])

    both_x, both_y = jnp.logical_and(low_x, high_x), jnp.logical_and(low_y, high_y)

    def await_sides(sem, planes, wide, corner):
        for nsx in (1, 2):
            for nsy in (1, 2):
                here = jnp.logical_and(both_x if nsx == 2 else jnp.logical_not(both_x),
                                       both_y if nsy == 2 else jnp.logical_not(both_y))
                total = planes * (nsx * wide * 8 + nsy * bx * wide + nsx * nsy * corner)
                ref = ballast.at[pl.ds(0, total)]

                @pl.when(here)
                def _():
                    pltpu.make_async_copy(ref, ref, sem).wait()

    def receive(g, o):
        await_sides(recv_sem.at[g % 2, o], 2, WIDTH, corner_cells)

    def clear(x0, nplanes, r0, nrows):
        def body(x, carry):
            for g in range(NB // GROUP):
                for o in range(norb):
                    us[GROUP * g][o, x, :, pl.ds(r0, nrows), :] = jnp.zeros((2, nrows, 128), jnp.float32)
            return carry
        lax.fori_loop(x0, x0 + nplanes, body, 0)

    def clear_pot(x0, nplanes, r0, nrows):
        pot[pl.ds(x0, nplanes), pl.ds(r0, nrows), :] = jnp.zeros((nplanes, nrows, 128), jnp.float32)

    for has, x0 in ((low_x, 0), (high_x, bx + WIDTH)):
        @pl.when(jnp.logical_not(has))
        def _():
            clear(x0, WIDTH, ROW - WIDTH, 8 + 2 * WIDTH)
            clear_pot(0 if x0 == 0 else bx + NEAR, NEAR, ROW - NEAR, 8 + 2 * NEAR)
    for has, r0 in ((low_y, ROW - WIDTH), (high_y, ROW + 8)):
        @pl.when(jnp.logical_not(has))
        def _():
            clear(0, bx + 2 * WIDTH, r0, WIDTH)
            clear_pot(0, bx + 2 * NEAR, ROW - NEAR if r0 < ROW else ROW + 8, NEAR)
    gram[...] = jnp.zeros_like(gram)

    load_pot.wait()

    def loaded(o):
        block = us[0].at[o, pl.ds(WIDTH, bx), :, rows]
        pltpu.make_async_copy(block, block, load_sem.at[1 + o]).wait()

    await_greetings(barrier, first)
    each_side(lambda side: pot_halo(side).start())
    for o in range(norb):
        loaded(o)
        send(0, o)
    greet(ready.at[0], rounds[0])

    zero, one = jnp.float32(0.0), jnp.float32(1.0)
    row = lax.broadcasted_iota(jnp.int32, (8, 128), 0)
    keep_rows = (
        jnp.where(jnp.logical_or(row >= ROW - RC, low_y), one, zero),
        jnp.where(jnp.logical_or(row < 8 - (ROW - RC), high_y), one, zero),
    )

    def coefficients(x, keep):
        for t in range(2):
            q = HALF_STEP * (DIAG + pot[x, pl.ds(RC + 8 * t, 8)])
            p = KAPPA / (1.0 + q * q) * keep_rows[t] * keep
            tile = pl.ds(8 * t, 8)
            qf[x, tile] = q
            pr[x, tile] = p
            pi[x, tile] = -q * p

    def weights(x, carry):
        q = HALF_STEP * (DIAG + pot[x + NEAR, rows])
        weight[x] = (1.0 + q * q) * (1.0 / KAPPA**2)
        return carry

    lax.fori_loop(0, bx, weights, 0, unroll=4)
    await_greetings(ready.at[0], rounds[0])
    greet(ready.at[1], rounds[1])
    await_sides(pot_sem.at[1], 1, NEAR, (NEAR - 2) ** 2)
    lax.fori_loop(0, NEAR, lambda x, c: (coefficients(x, jnp.where(low_x, one, zero)), c)[1], 0)
    lax.fori_loop(NEAR, bx + NEAR, lambda x, c: (coefficients(x, one), c)[1], 0, unroll=4)
    lax.fori_loop(bx + NEAR, bx + 2 * NEAR, lambda x, c: (coefficients(x, jnp.where(high_x, one, zero)), c)[1], 0)

    lane = lax.broadcasted_iota(jnp.int32, (8, 128), 1)
    near = (jnp.where(lane >= 1, one, zero), jnp.where(lane < 127, one, zero))
    far = (jnp.where(lane >= 2, FAR * one, zero), jnp.where(lane < 126, FAR * one, zero))

    def stencil(u, o, x, c, r):
        def at(dx, dr):
            return u[o, x + WIDTH + dx, c, pl.ds(r + dr, 8)]
        center = at(0, 0)
        s1 = (at(-1, 0) + at(1, 0)) + (at(0, -1) + at(0, 1))
        s2 = (at(-2, 0) + at(2, 0)) + (at(0, -2) + at(0, 2))
        z1 = near[0] * pltpu.roll(center, 1, 1) + near[1] * pltpu.roll(center, 127, 1)
        z2 = far[0] * pltpu.roll(center, 2, 1) + far[1] * pltpu.roll(center, 126, 1)
        return center, (s1 + z1) + (FAR * s2 + z2)

    def advance(s, o):
        u, margin = us[s], WIDTH - 2 - 2 * (s % GROUP)
        for x in range(-margin, bx + margin):
            out = -x if x < 0 else x - bx + 1 if x >= bx else 0
            beyond = margin - 2 * ((out + 1) // 2)
            for r in (ROW,) if beyond == 0 else (RC, RC + 8):
                u_re, t_re = stencil(u, o, x, 0, r)
                u_im, t_im = stencil(u, o, x, 1, r)
                tile = pl.ds(r - RC, 8)
                a, b = pr[x + NEAR, tile], pi[x + NEAR, tile]
                if s == 0:
                    q = qf[x + NEAR, tile]
                    w_re = 2.0 * (KAPPA * t_im + q * u_im)
                    w_im = -2.0 * (KAPPA * t_re + q * u_re)
                    v_re, v_im = a * w_re - b * w_im, a * w_im + b * w_re
                else:
                    re, im = SHIFT[s]
                    v_re, v_im = -(a * t_im + b * t_re), a * t_re - b * t_im
                    if re != 0.0:
                        v_re = (im * u_im - a * t_im) - (re * u_re + b * t_re)
                        v_im = (a * t_re - re * u_im) - (im * u_re + b * t_im)
                us[s + 1][o, x + WIDTH, 0, pl.ds(r, 8)] = v_re
                us[s + 1][o, x + WIDTH, 1, pl.ds(r, 8)] = v_im

    def vector(k, o, x):
        return us[k + 1][o, x + WIDTH, 0, rows], us[k + 1][o, x + WIDTH, 1, rows]

    def products(o, pairs):
        acc = {}
        for x in range(bx):
            v = {k: vector(k, o, x) for k in sorted({k for pair in pairs for k in pair})}
            weighted = {i: (weight[x] * v[i][0], weight[x] * v[i][1]) for i in sorted({i for i, _ in pairs})}
            for i, j in pairs:
                (ar, ai), (br, bi) = weighted[i], v[j]
                terms = [ar * br + ai * bi] + ([ar * bi - ai * br] if i != j else [])
                for part, term in enumerate(terms):
                    key = (i, j, part, x % 2)
                    acc[key] = acc[key] + term if key in acc else term
        for i, j in pairs:
            for part in range(1 if i == j else 2):
                tile = acc[i, j, part, 0] + acc[i, j, part, 1]
                gram[o, pl.ds(part * IM + tri(i, j), 1)] = jnp.sum(tile, axis=0, keepdims=True)

    def column_products(g, o):
        new = range(GROUP * g, GROUP * g + GROUP)
        for i in range(GROUP * g):
            products(o, [(i, j) for j in new])
        products(o, [(i, j) for i in new for j in new if i <= j][:3])
        products(o, [(i, j) for i in new for j in new if i <= j][3:])

    def exchange(part, me, n, target, ssem, rsem):
        def start(o, row):
            part[o, me] = row
            for d in sorted(range(1, n), key=lambda d: -min(d, n - d)):
                pltpu.make_async_remote_copy(
                    src_ref=part.at[o, me], dst_ref=part.at[o, me], send_sem=ssem, recv_sem=rsem.at[o],
                    device_id=target(lax.rem(me + d, n)), device_id_type=MESH,
                ).start()

        def total(o):
            others = part.at[o, pl.ds(0, n - 1)]
            pltpu.make_async_copy(others, others, rsem.at[o]).wait()
            terms = [part[o, k] for k in range(n)]
            while len(terms) > 1:
                terms = [terms[k] + terms[k + 1] for k in range(0, len(terms), 2)]
            return terms[0]

        def drain():
            others = part.at[:, pl.ds(0, n - 1)]
            pltpu.make_async_copy(others, others, ssem).wait()

        return start, total, drain

    start_y, total_y, drain_y = exchange(part_y, iy, ny, lambda t: (io, ix, t), ysend_sem.at[0], yrecv_sem)
    start_x, total_x, drain_x = exchange(part_x, ix, nx, lambda t: (io, t, iy), xsend_sem.at[0], xrecv_sem)

    def start_reduction(o):
        sums = lax.dot_general(
            jnp.ones((8, 128), jnp.float32), gram[o], (((1,), (1,)), ((), ())),
            precision=lax.Precision.HIGHEST, preferred_element_type=jnp.float32,
        )
        start_y(o, sums[0:1])

    groups = NB // GROUP
    for g in range(groups):
        def orbital(o, carry):
            receive(g, o)
            for s in range(GROUP * g, GROUP * g + GROUP):
                advance(s, o)
            if g < groups - 1:
                send(g + 1, o)
            else:
                column_products(g, o)
                start_reduction(o)
            return carry
        lax.fori_loop(0, norb, orbital, 0)
        if g == 0:
            await_greetings(ready.at[1], rounds[1])
            greet(ready.at[2], rounds[2])
        if g == 1:
            await_greetings(ready.at[2], rounds[2])
        if g < groups - 1:
            def gram_columns(o, carry):
                column_products(g, o)
                return carry
            lax.fori_loop(0, norb, gram_columns, 0)

    def second_stage(o, carry):
        start_x(o, total_y(o))
        return carry

    lax.fori_loop(0, norb, second_stage, 0)

    await_sides(pot_sem.at[0], 1, NEAR, (NEAR - 2) ** 2)
    for side, (dx, dy) in enumerate(sides):
        cells = sum(sx.size * sr.size for (sx, _), (sr, _) in halo_spans(side))
        sent = ux.at[:, :, pl.ds(0, cells // 4), :, pl.ds(ROW, 4)]

        @pl.when(present(dx, dy))
        def _():
            pltpu.make_async_copy(sent, sent, send_sem.at[side]).wait()
    drain_y()

    def finish(o, carry):
        total = jnp.broadcast_to(total_x(o), (8, 128))

        def spread(e):
            return jnp.broadcast_to(total[:, e:e + 1], (8, 128))

        entries = {}
        for j in range(NB):
            for i in range(j + 1):
                re = spread(tri(i, j))
                im = jnp.zeros_like(re) if i == j else spread(IM + tri(i, j))
                entries[i, j] = (re, im)
                if i != j:
                    entries[j, i] = (re, -im)
        res_coef, x_coef = recurrences(lambda i, j: entries[i, j])
        rc = [(c[0] * (1.0 / KAPPA), c[1] * (1.0 / KAPPA)) for c in res_coef]
        xc = [(c[0] * (1.0 / KAPPA), c[1] * (1.0 / KAPPA)) for c in x_coef]

        def combine(x, carry):
            vectors = [vector(k, o, x) for k in range(NB)]
            re, im = csum([cmul(rc[k], vectors[k]) for k in range(NB)])
            inc = csum([cmul(xc[k], vectors[k]) for k in range(NB - 1)])
            q = qf[x + NEAR, pl.ds(ROW - RC, 8)]
            out_ref[1, 0, o, x] = re - q * im
            out_ref[1, 1, o, x] = im + q * re
            for c in range(2):
                out_ref[0, c, o, x] = us[0][o, x + WIDTH, c, rows] + inc[c]
            return carry

        lax.fori_loop(0, bx, combine, 0, unroll=4)
        return carry

    lax.fori_loop(0, norb, finish, 0)
    drain_x()


def solution(mesh):
    nx, ny = mesh.shape["gx"], mesh.shape["gyz"]

    def shards(orbitals, potential):
        _, norb, bx, by, nz = orbitals.shape
        both = pl.pallas_call(
            functools.partial(kernel, nx, ny),
            out_shape=jax.ShapeDtypeStruct((2, *orbitals.shape), jnp.float32),
            in_specs=[pl.BlockSpec(memory_space=pltpu.HBM)] * 2,
            out_specs=pl.BlockSpec(memory_space=pltpu.VMEM),
            scratch_shapes=[
                pltpu.VMEM((NB // GROUP, norb, bx + 2 * WIDTH, 2, by + 16, nz), jnp.float32)
            ] + [
                pltpu.VMEM((norb, bx + 2 * WIDTH, 2, by + 16, nz), jnp.float32) for _ in range(NB + 1 - NB // GROUP)
            ] + [
                pltpu.VMEM((bx + 2 * NEAR, by + 16, nz), jnp.float32),
                pltpu.VMEM((4 * (WIDTH * 8 + bx * WIDTH + 2 * NEAR * NEAR), nz), jnp.float32),
                pltpu.VMEM((bx + 2 * NEAR, 16, nz), jnp.float32),
                pltpu.VMEM((bx + 2 * NEAR, 16, nz), jnp.float32),
                pltpu.VMEM((bx + 2 * NEAR, 16, nz), jnp.float32),
                pltpu.VMEM((bx, by, nz), jnp.float32),
                pltpu.VMEM((norb, 128, 128), jnp.float32),
                pltpu.VMEM((norb, ny, 1, 128), jnp.float32),
                pltpu.VMEM((norb, nx, 1, 128), jnp.float32),
                pltpu.SemaphoreType.REGULAR((NB // GROUP,)),
                pltpu.SemaphoreType.DMA((1 + norb,)),
                pltpu.SemaphoreType.DMA((2,)),
                pltpu.SemaphoreType.DMA((8,)),
                pltpu.SemaphoreType.DMA((2, norb)),
                pltpu.SemaphoreType.DMA((1,)),
                pltpu.SemaphoreType.DMA((norb,)),
                pltpu.SemaphoreType.DMA((1,)),
                pltpu.SemaphoreType.DMA((norb,)),
            ],
            compiler_params=pltpu.CompilerParams(
                collective_id=0, has_side_effects=True, vmem_limit_bytes=48 * 2**20
            ),
        )(*(pltpu.with_memory_space_constraint(a, pltpu.HBM) for a in (orbitals, potential)))
        return both[0], both[1]

    spec = P(None, "orb", "gx", "gyz", None)
    return jax.shard_map(
        shards, mesh=mesh, in_specs=(spec, P("gx", "gyz", None)), out_specs=(spec, spec), check_vma=False
    )
```
